768 devices in a mesh: blk: 192 (over z_hi, x, y, core), grp: 4 (over z_lo).
Axes of the slice: x: 4, y: 8, z: 12 (z_hi: 3, z_lo: 4; z = z_hi * 4 + z_lo), core: 2. Of those that a mesh axis runs over, the one named last changes fastest.
Arguments:
- image_embeds: bfloat16 [98304, 1152], P(('blk', 'grp')), may hold values from -6 to 6
- text_embeds: bfloat16 [98304, 1152], P(('blk', 'grp')), may hold values from -6 to 6
Outputs:
- image_embed_gradient: bfloat16 [98304, 1152], P(('blk', 'grp'))
- text_embed_gradient: bfloat16 [98304, 1152], P(('blk', 'grp'))
The draws below stay inside these ranges and needn't reach their ends.
All inputs are finite; a program needn't handle non-finite values.
Results may differ from the reference program's by a relative error of at most 0.0059.
Values may be sent and summed in bfloat16 or wider, within the bound.
A program may use at most 64 MiB of HBM per device.

```python
import jax
import jax.numpy as jnp
from jax import lax

EMBED_WIDTH = 1152
BLOCK_ROWS = 128
STEPS = 20
BATCH = 98304


def block_scale(rng, dims, cuts, smallest, largest):
    def one(position, blocks):
        heights = jax.random.uniform(jax.random.fold_in(jax.random.fold_in(rng, 6), position), (blocks,), jnp.float32, smallest / len(cuts), largest / len(cuts))
        return jnp.repeat(jnp.exp(heights), dims[position] // blocks).reshape((-1,) + (1,) * (len(dims) - position - 1))

    loudness = one(*cuts[0])
    for cut in cuts[1:]:
        loudness = loudness * one(*cut)
    return loudness


def gaussian(key, extent, scale, reach, split=(), held_as=jnp.bfloat16):
    drawn = scale * jax.random.normal(key, extent, jnp.float32)
    if split:
        drawn = drawn * block_scale(key, extent, split, -0.22, 0.18)
    return jnp.clip(drawn, -reach, reach).astype(held_as)


def setup_inputs(seed: int = 0) -> dict:
    seeds = jax.random.split(jax.random.key(seed), 3)
    return {
        "image_embeds": gaussian(seeds[0], (BATCH, EMBED_WIDTH), 1.0, 6.0, ((0, 768),)),
        "text_embeds": gaussian(seeds[1], (BATCH, EMBED_WIDTH), 1.0, 6.0, ((0, 768),)),
    }


LOGIT_SCALE = 10.0
BIAS_LOGIT = -2.0
EPSILON = 1e-06

def normalize(values):
    wide = values.astype(jnp.float32)
    length = jnp.sqrt(lax.optimization_barrier(jnp.sum(wide * wide, axis=-1, keepdims=True)) + EPSILON)
    return (wide / length, length)

def undo_normalization(grad, unit, length):
    inner = lax.optimization_barrier(jnp.sum(unit * grad, axis=-1, keepdims=True))
    return (grad - unit * inner) / length

def pair_weights(pair_logits, is_first):
    count = pair_logits.shape[-1]
    diagonal_mask = jnp.eye(count, dtype=bool) & is_first
    return jnp.where(diagonal_mask, -jax.nn.sigmoid(-pair_logits), jax.nn.sigmoid(pair_logits))

def reference(image_embeds, text_embeds):
    block_list = image_embeds.shape[0] // BLOCK_ROWS
    image_normalized, image_norm = normalize(image_embeds)
    text_normalized, text_norm = normalize(text_embeds)
    image_reduced = image_normalized.astype(jnp.bfloat16).astype(jnp.float32).reshape(block_list, BLOCK_ROWS, EMBED_WIDTH)
    text_low = text_normalized.astype(jnp.bfloat16).astype(jnp.float32).reshape(block_list, BLOCK_ROWS, EMBED_WIDTH)

    def advance(running, offset):
        image_total, text_total = running
        shifted_block = jnp.roll(text_low, offset, axis=0)
        pair_logits = LOGIT_SCALE * jnp.einsum('gty,gky->gtk', image_reduced, shifted_block) + BIAS_LOGIT
        weights = pair_weights(pair_logits, offset == 0).astype(jnp.bfloat16).astype(jnp.float32)
        image_total = image_total + jnp.einsum('prc,pcd->prd', weights, shifted_block)
        text_terms = jnp.einsum('prc,prd->pcd', weights, image_reduced)
        text_total = text_total + jnp.roll(text_terms, -offset, axis=0)
        return ((image_total, text_total), None)
    zeros = jnp.zeros((block_list, BLOCK_ROWS, EMBED_WIDTH), jnp.float32)
    (image_total, text_total), _ = lax.scan(advance, (zeros, zeros), jnp.arange(STEPS, dtype=jnp.int32))
    image_gradient = LOGIT_SCALE * image_total.reshape(block_list * BLOCK_ROWS, EMBED_WIDTH)
    text_gradient = LOGIT_SCALE * text_total.reshape(block_list * BLOCK_ROWS, EMBED_WIDTH)
    image_embed_gradient = undo_normalization(image_gradient, image_normalized, image_norm).astype(jnp.bfloat16)
    text_embed_gradient = undo_normalization(text_gradient, text_normalized, text_norm).astype(jnp.bfloat16)
    return (image_embed_gradient, text_embed_gradient)
```

```python
import jax
import jax.numpy as jnp
from jax import lax
from jax.experimental import pallas as pl
from jax.experimental.pallas import tpu as pltpu
from jax.sharding import PartitionSpec as P

MESH = pl.DeviceIdType.MESH
LOGIT_SCALE = 10.0
BIAS_LOGIT = -2.0
EPSILON = 1e-06
ROWS = 128
WIDTH = 1152
CHUNKS = 2
PIECE = ROWS // CHUNKS
COLS = 384
F32 = jnp.float32
BF16 = jnp.bfloat16


def unit_and_inverse(ref):
    wide = ref[...].astype(F32)
    length = jnp.sqrt(jnp.sum(wide * wide, axis=-1, keepdims=True) + EPSILON)
    inverse = 1.0 / length
    return wide * inverse, inverse


def undo(total, ref):
    unit, inverse = unit_and_inverse(ref)
    grad = LOGIT_SCALE * total
    inner = jnp.sum(unit * grad, axis=-1, keepdims=True)
    return ((grad - unit * inner) * inverse).astype(BF16)


def kernel(
    blocks,
    image_ref, text_ref, image_out, text_out,
    img, txt, wgt, q_sum, p_sum,
    q_send, q_recv, far_out, near_out, near_in, far_in, p_send, p_recv,
    txt_ssem, txt_rsem, img_fsem, img_nsem, img_psem, img_rsem,
    q_ssem, q_rsem, far_ssem, near_ssem, near_rsem, far_rsem, p_ssem, p_rsem,
):
    blk = lax.axis_index("blk")
    z = lax.axis_index("grp")
    k = lax.rem(blk, 2)
    j = 4 * k + z
    high = z // 2
    sign = 1 - 2 * high
    middle = (z == 1) | (z == 2)
    edge = (z == 0) | (z == 3)

    def spot(t):
        return 3 * high + sign * t

    partner = (blk + 1 - 2 * k, z)
    ahead = (lax.rem(blk + 2, blocks), z)
    behind = (lax.rem(blk + blocks - 2, blocks), z)
    far = (blk, z + sign)
    near = (blk, z - sign)

    def copy(src, dst, ssem, rsem, device):
        return pltpu.make_async_remote_copy(
            src_ref=src, dst_ref=dst, send_sem=ssem, recv_sem=rsem, device_id=device, device_id_type=MESH
        )

    def rows(h):
        return pl.ds(h * PIECE, PIECE)

    barrier = pltpu.get_barrier_semaphore()
    for device in (partner, ahead, behind, far):
        pl.semaphore_signal(barrier, inc=1, device_id=device, device_id_type=MESH)

    @pl.when(middle)
    def _():
        pl.semaphore_signal(barrier, inc=1, device_id=near, device_id_type=MESH)

    unit, _ = unit_and_inverse(image_ref)
    img[k, z] = unit.astype(BF16)
    unit, _ = unit_and_inverse(text_ref)
    txt[0] = unit.astype(BF16)

    pl.semaphore_wait(barrier, 4 + z * (3 - z) // 2)

    def image_copy(t, h, ssem, device):
        s = spot(t)
        ref = img.at[k, s, rows(h)]
        return copy(ref, ref, ssem.at[t, h], img_rsem.at[k, s, h], device)

    def image_arrival(kk, s, h):
        ref = img.at[kk, s, rows(h)]
        copy(ref, ref, img_psem.at[0, h], img_rsem.at[kk, s, h], partner).wait_recv()

    def text_copy(d, h):
        return copy(
            txt.at[d, rows(h)], txt.at[d + 1, rows(h)], txt_ssem.at[d, h], txt_rsem.at[d, h], ahead
        )

    def text_arrival(d, h):
        copy(
            txt.at[d, rows(h)], txt.at[d + 1, rows(h)], txt_ssem.at[d, h], txt_rsem.at[d, h], ahead
        ).wait_recv()

    for h in range(CHUNKS):
        text_copy(0, h).start()

        @pl.when(edge)
        def _():
            image_copy(0, h, img_fsem, far).start()
            image_copy(0, h, img_psem, partner).start()

        @pl.when(middle)
        def _():
            image_copy(1, h, img_fsem, far).start()
            image_copy(1, h, img_nsem, near).start()
            image_copy(1, h, img_psem, partner).start()

    for u in range(3):
        for h in range(CHUNKS):
            @pl.when(edge)
            def _():
                image_arrival(k, spot(u + 1), h)
                image_copy(u + 1, h, img_psem, partner).start()

            @pl.when(middle)
            def _():
                if u == 0:
                    image_arrival(k, spot(0), h)
                    image_copy(0, h, img_fsem, far).start()
                    image_copy(0, h, img_psem, partner).start()
                else:
                    image_arrival(k, spot(u + 1), h)
                    image_copy(u + 1, h, img_nsem, near).start()
                    image_copy(u + 1, h, img_psem, partner).start()

            if u < 2:
                text_arrival(u, h)
                if u == 0:
                    text_copy(1, h).start()
                else:
                    @pl.when(j >= 5)
                    def _():
                        text_copy(2, h).start()
            else:
                @pl.when(j >= 5)
                def _():
                    text_arrival(2, h)

    @pl.when(j < 5)
    def _():
        txt[3] = jnp.zeros((ROWS, WIDTH), BF16)

    for s in range(4):
        for h in range(CHUNKS):
            image_arrival(1 - k, s, h)

    p_sum[...] = jnp.zeros_like(p_sum)

    @pl.loop(0, 4)
    def _(s):
        pair = img[:, s].reshape(2 * ROWS, WIDTH)
        texts = txt[...].reshape(4 * ROWS, WIDTH)
        logits = (
            LOGIT_SCALE
            * lax.dot_general(pair, texts, (((1,), (1,)), ((), ())), preferred_element_type=F32)
            + BIAS_LOGIT
        )
        row = lax.broadcasted_iota(jnp.int32, logits.shape, 0)
        col = lax.broadcasted_iota(jnp.int32, logits.shape, 1)
        gap = 8 * (col // ROWS) + 4 * (row // ROWS) + (s - j)
        match = (gap == 0) & (lax.rem(row, ROWS) == lax.rem(col, ROWS))
        weight = jax.nn.sigmoid(jnp.where(match, -logits, logits))
        weight = jnp.where(match, -weight, weight)
        weight = jnp.where((gap >= 0) & (gap <= 19), weight, 0.0)
        wgt[...] = weight.astype(BF16)
        for n in range(WIDTH // COLS):
            part = pl.ds(n * COLS, COLS)
            texts = txt[:, :, part].reshape(4 * ROWS, COLS)
            q = jnp.dot(wgt[...], texts, preferred_element_type=F32)
            q_sum[:, s, :, part] = q.reshape(2, ROWS, COLS)
            pair = img[:, s, :, part].reshape(2 * ROWS, COLS)
            p = lax.dot_general(wgt[...], pair, (((0,), (0,)), ((), ())), preferred_element_type=F32)
            p_sum[:, :, part] += p.reshape(4, ROWS, COLS)
        q_send[s] = q_sum[1 - k, s].astype(BF16)
        copy(q_send.at[s], q_recv.at[s], q_ssem.at[s], q_rsem.at[s], partner).start()

    def back_copy(d, h):
        return copy(p_send.at[d, rows(h)], p_recv.at[d, rows(h)], p_ssem.at[d, h], p_rsem.at[d, h], behind)

    def far_copy(t, h, receiver):
        s = spot(t)
        sem = {"near": near_rsem, "far": far_rsem}[receiver]
        dst = {"near": near_in, "far": far_in}[receiver]
        return copy(far_out.at[s, rows(h)], dst.at[s, rows(h)], far_ssem.at[s, h], sem.at[s, h], far)

    def near_copy(h):
        s = spot(0)
        return copy(near_out.at[rows(h)], far_in.at[s, rows(h)], near_ssem.at[h], far_rsem.at[s, h], near)

    def near_arrival(t, h):
        s = spot(t)
        copy(far_out.at[s, rows(h)], near_in.at[s, rows(h)], far_ssem.at[s, h], near_rsem.at[s, h], far).wait_recv()

    def far_arrival(t, h):
        s = spot(t)
        copy(far_out.at[s, rows(h)], far_in.at[s, rows(h)], far_ssem.at[s, h], far_rsem.at[s, h], far).wait_recv()

    @pl.when(j >= 5)
    def _():
        p_send[2] = p_sum[3].astype(BF16)
        for h in range(CHUNKS):
            back_copy(2, h).start()

    @pl.loop(0, 4)
    def _(s):
        copy(q_send.at[s], q_recv.at[s], q_ssem.at[s], q_rsem.at[s], partner).wait_recv()

    for u in range(3):
        for h in range(CHUNKS):
            r = rows(h)

            @pl.when(edge)
            def _():
                t = spot(3 - u)
                far_out[t, r] = (q_sum[k, t, r] + q_recv[t, r].astype(F32)).astype(BF16)
                far_copy(3 - u, h, "near").start()

            if u < 2:
                @pl.when(middle)
                def _():
                    t = spot(3 - u)
                    near_arrival(3 - u, h)
                    total = q_sum[k, t, r] + q_recv[t, r].astype(F32) + near_in[t, r].astype(F32)
                    far_out[t, r] = total.astype(BF16)
                    far_copy(3 - u, h, "far").start()

            if u == 1:
                @pl.when(middle)
                def _():
                    t = spot(0)
                    far_arrival(0, h)
                    total = q_sum[k, t, r] + q_recv[t, r].astype(F32) + far_in[t, r].astype(F32)
                    near_out[r] = total.astype(BF16)
                    near_copy(h).start()

            if u == 0:
                @pl.when(j >= 5)
                def _():
                    copy(p_send.at[2, r], p_recv.at[2, r], p_ssem.at[2, h], p_rsem.at[2, h], behind).wait_recv()
                    p_send[1, r] = (p_sum[2, r] + p_recv[2, r].astype(F32)).astype(BF16)
                    back_copy(1, h).start()

                @pl.when(j < 5)
                def _():
                    p_send[1, r] = p_sum[2, r].astype(BF16)
                    back_copy(1, h).start()

            if u == 1:
                copy(p_send.at[1, r], p_recv.at[1, r], p_ssem.at[1, h], p_rsem.at[1, h], behind).wait_recv()
                p_send[0, r] = (p_sum[1, r] + p_recv[1, r].astype(F32)).astype(BF16)
                back_copy(0, h).start()

    for h in range(CHUNKS):
        r = rows(h)
        copy(p_send.at[0, r], p_recv.at[0, r], p_ssem.at[0, h], p_rsem.at[0, h], behind).wait_recv()
    text_out[...] = undo(p_sum[0] + p_recv[0].astype(F32), text_ref)

    @pl.when(edge)
    def _():
        for h in range(CHUNKS):
            far_arrival(0, h)
        total = q_sum[k, z] + q_recv[z].astype(F32) + far_in[z].astype(F32)
        image_out[...] = undo(total, image_ref)

    @pl.when(middle)
    def _():
        for h in range(CHUNKS):
            near_arrival(1, h)
            far_arrival(1, h)
        total = q_sum[k, z] + q_recv[z].astype(F32) + near_in[z].astype(F32) + far_in[z].astype(F32)
        image_out[...] = undo(total, image_ref)

    for h in range(CHUNKS):
        text_copy(0, h).wait_send()
        text_copy(1, h).wait_send()
        back_copy(0, h).wait_send()
        back_copy(1, h).wait_send()

        @pl.when(j >= 5)
        def _():
            text_copy(2, h).wait_send()
            back_copy(2, h).wait_send()

        for t in range(4):
            image_copy(t, h, img_psem, partner).wait_send()

        @pl.when(edge)
        def _():
            image_copy(0, h, img_fsem, far).wait_send()
            for t in (1, 2, 3):
                far_copy(t, h, "near").wait_send()

        @pl.when(middle)
        def _():
            for t in (0, 1):
                image_copy(t, h, img_fsem, far).wait_send()
            for t in (1, 2, 3):
                image_copy(t, h, img_nsem, near).wait_send()
            for t in (2, 3):
                far_copy(t, h, "far").wait_send()
            near_copy(h).wait_send()

    @pl.loop(0, 4)
    def _(s):
        copy(q_send.at[s], q_recv.at[s], q_ssem.at[s], q_rsem.at[s], partner).wait_send()


def solution(mesh):
    blocks = mesh.shape["blk"]
    dma = pltpu.SemaphoreType.DMA
    block = (ROWS, WIDTH)

    def per_device(image_embeds, text_embeds):
        out = jax.ShapeDtypeStruct(block, BF16)
        vmem = pl.BlockSpec(memory_space=pltpu.VMEM)
        return pl.pallas_call(
            lambda *refs: kernel(blocks, *refs),
            out_shape=(out, out),
            in_specs=[vmem, vmem],
            out_specs=(vmem, vmem),
            scratch_shapes=[
                pltpu.VMEM((2, 4) + block, BF16),
                pltpu.VMEM((4,) + block, BF16),
                pltpu.VMEM((2 * ROWS, 4 * ROWS), BF16),
                pltpu.VMEM((2, 4) + block, F32),
                pltpu.VMEM((4,) + block, F32),
                pltpu.VMEM((4,) + block, BF16),
                pltpu.VMEM((4,) + block, BF16),
                pltpu.VMEM((4,) + block, BF16),
                pltpu.VMEM(block, BF16),
                pltpu.VMEM((4,) + block, BF16),
                pltpu.VMEM((4,) + block, BF16),
                pltpu.VMEM((3,) + block, BF16),
                pltpu.VMEM((3,) + block, BF16),
                dma((3, CHUNKS)),
                dma((3, CHUNKS)),
                dma((4, CHUNKS)),
                dma((4, CHUNKS)),
                dma((4, CHUNKS)),
                dma((2, 4, CHUNKS)),
                dma((4,)),
                dma((4,)),
                dma((4, CHUNKS)),
                dma((CHUNKS,)),
                dma((4, CHUNKS)),
                dma((4, CHUNKS)),
                dma((3, CHUNKS)),
                dma((3, CHUNKS)),
            ],
            compiler_params=pltpu.CompilerParams(
                collective_id=0, has_side_effects=True, vmem_limit_bytes=56 * 1024 * 1024
            ),
            name="pair_window",
        )(image_embeds, text_embeds)

    spec = P(("blk", "grp"), None)
    return jax.shard_map(
        per_device, mesh=mesh, in_specs=(spec, spec), out_specs=(spec, spec), check_vma=False
    )
```

```python
import jax
import jax.numpy as jnp
from jax import lax
from jax.experimental import pallas as pl
from jax.experimental.pallas import tpu as pltpu
from jax.sharding import PartitionSpec as P

MESH = pl.DeviceIdType.MESH
LOGIT_SCALE = 10.0
BIAS_LOGIT = -2.0
EPSILON = 1e-06
ROWS = 128
WIDTH = 1152
CHUNKS = 2
PIECE = ROWS // CHUNKS
SLICES = 4
THIN = ROWS // SLICES
RELAYS = ((24, 7, 1, 30), (23, 8, 15, 16))
COLS = 384
F32 = jnp.float32
BF16 = jnp.bfloat16


def unit_and_inverse(ref):
    wide = ref[...].astype(F32)
    length = jnp.sqrt(jnp.sum(wide * wide, axis=-1, keepdims=True) + EPSILON)
    inverse = 1.0 / length
    return wide * inverse, inverse


def undo(total, ref):
    unit, inverse = unit_and_inverse(ref)
    grad = LOGIT_SCALE * total
    inner = jnp.sum(unit * grad, axis=-1, keepdims=True)
    return ((grad - unit * inner) * inverse).astype(BF16)


def kernel(
    blocks,
    image_ref, text_ref, image_out, text_out,
    img, txt, wgt, q_sum, p_sum,
    q_send, q_recv, far_out, near_out, near_in, far_in, p_send, p_recv,
    fwd_hold, back_hold,
    txt_ssem, txt_rsem, img_fsem, img_nsem, img_psem, img_rsem,
    q_ssem, q_rsem, far_ssem, near_ssem, near_rsem, far_rsem, p_ssem, p_rsem,
    fwd_ssem, fwd_rsem, back_ssem, back_rsem,
):
    blk = lax.axis_index("blk")
    z = lax.axis_index("grp")
    k = lax.rem(blk, 2)
    j = 4 * k + z
    high = z // 2
    sign = 1 - 2 * high
    middle = (z == 1) | (z == 2)
    edge = (z == 0) | (z == 3)

    def spot(t):
        return 3 * high + sign * t

    column = blk // 2
    third = column // 32
    place = lax.rem(column, 32)
    first = place == 0
    last = place == 31

    def relay_place(h):
        return RELAYS[0][h] + k * (RELAYS[1][h] - RELAYS[0][h])

    def at(hop, where):
        return (2 * (32 * lax.rem(third + hop, blocks // 64) + where) + k, z)

    is_role = [jnp.where(place == relay_place(h), 1, 0) for h in range(SLICES)]
    role = is_role[1] + 2 * is_role[2] + 3 * is_role[3]
    relay = is_role[0] + is_role[1] + is_role[2] + is_role[3] > 0
    next_first, own_first = at(1, 0), at(0, 0)
    prev_last, own_last = at(blocks // 64 - 1, 31), at(0, 31)

    partner = (blk + 1 - 2 * k, z)
    ahead = (lax.rem(blk + 2, blocks), z)
    behind = (lax.rem(blk + blocks - 2, blocks), z)
    far = (blk, z + sign)
    near = (blk, z - sign)

    def copy(src, dst, ssem, rsem, device):
        return pltpu.make_async_remote_copy(
            src_ref=src, dst_ref=dst, send_sem=ssem, recv_sem=rsem, device_id=device, device_id_type=MESH
        )

    def rows(h):
        return pl.ds(h * PIECE, PIECE)

    def thin(h):
        return pl.ds(pl.multiple_of(h * THIN, THIN), THIN)

    barrier = pltpu.get_barrier_semaphore()
    for device in (partner, ahead, behind, far):
        pl.semaphore_signal(barrier, inc=1, device_id=device, device_id_type=MESH)

    @pl.when(middle)
    def _():
        pl.semaphore_signal(barrier, inc=1, device_id=near, device_id_type=MESH)

    @pl.when(relay)
    def _():
        for device in (next_first, own_first, prev_last, own_last):
            pl.semaphore_signal(barrier, inc=1, device_id=device, device_id_type=MESH)

    @pl.when(first)
    def _():
        for h in range(SLICES):
            for device in (at(0, relay_place(h)), at(blocks // 64 - 1, relay_place(h))):
                pl.semaphore_signal(barrier, inc=1, device_id=device, device_id_type=MESH)

    @pl.when(last)
    def _():
        for h in range(SLICES):
            for device in (at(0, relay_place(h)), at(1, relay_place(h))):
                pl.semaphore_signal(barrier, inc=1, device_id=device, device_id_type=MESH)

    unit, _ = unit_and_inverse(image_ref)
    img[k, z] = unit.astype(BF16)
    unit, _ = unit_and_inverse(text_ref)
    txt[0] = unit.astype(BF16)

    greeted = 4 + z * (3 - z) // 2 + jnp.where(relay, 4, 0) + jnp.where(first | last, 2 * SLICES, 0)
    pl.semaphore_wait(barrier, greeted)

    def image_copy(t, h, ssem, device):
        s = spot(t)
        ref = img.at[k, s, rows(h)]
        return copy(ref, ref, ssem.at[t, h], img_rsem.at[k, s, h], device)

    def image_arrival(kk, s, h):
        ref = img.at[kk, s, rows(h)]
        copy(ref, ref, img_psem.at[0, h], img_rsem.at[kk, s, h], partner).wait_recv()

    def text_copy(d, h):
        return copy(
            txt.at[d, thin(h)], txt.at[d + 1, thin(h)], txt_ssem.at[d, h], txt_rsem.at[d, h], ahead
        )

    def text_start(d, h):
        @pl.when(last)
        def _():
            copy(
                txt.at[d, thin(h)], fwd_hold.at[d], txt_ssem.at[d, h], fwd_rsem.at[d], at(0, relay_place(h))
            ).start()

        @pl.when(jnp.logical_not(last))
        def _():
            text_copy(d, h).start()

    def text_relay(d):
        return copy(
            fwd_hold.at[d], txt.at[d + 1, thin(role)], fwd_ssem.at[d], txt_rsem.at[d, role], next_first
        )

    def text_relay_stage(d):
        @pl.when(relay & (j >= 5) if d == 2 else relay)
        def _():
            copy(fwd_hold.at[d], fwd_hold.at[d], fwd_ssem.at[d], fwd_rsem.at[d], next_first).wait_recv()
            text_relay(d).start()

    for h in range(SLICES):
        text_start(0, h)

    for h in range(CHUNKS):
        @pl.when(edge)
        def _():
            image_copy(0, h, img_fsem, far).start()
            image_copy(0, h, img_psem, partner).start()

        @pl.when(middle)
        def _():
            image_copy(1, h, img_fsem, far).start()
            image_copy(1, h, img_nsem, near).start()
            image_copy(1, h, img_psem, partner).start()

    for u in range(3):
        text_relay_stage(u)
        for h in range(CHUNKS):
            @pl.when(edge)
            def _():
                image_arrival(k, spot(u + 1), h)
                image_copy(u + 1, h, img_psem, partner).start()

            @pl.when(middle)
            def _():
                if u == 0:
                    image_arrival(k, spot(0), h)
                    image_copy(0, h, img_fsem, far).start()
                    image_copy(0, h, img_psem, partner).start()
                else:
                    image_arrival(k, spot(u + 1), h)
                    image_copy(u + 1, h, img_nsem, near).start()
                    image_copy(u + 1, h, img_psem, partner).start()

        if u < 2:
            for h in range(SLICES):
                text_copy(u, h).wait_recv()
                if u == 0:
                    text_start(1, h)
                else:
                    @pl.when(j >= 5)
                    def _():
                        text_start(2, h)
        else:
            @pl.when(j >= 5)
            def _():
                for h in range(SLICES):
                    text_copy(2, h).wait_recv()

    @pl.when(j < 5)
    def _():
        txt[3] = jnp.zeros((ROWS, WIDTH), BF16)

    for s in range(4):
        for h in range(CHUNKS):
            image_arrival(1 - k, s, h)

    p_sum[...] = jnp.zeros_like(p_sum)

    @pl.loop(0, 4)
    def _(s):
        pair = img[:, s].reshape(2 * ROWS, WIDTH)
        texts = txt[...].reshape(4 * ROWS, WIDTH)
        logits = (
            LOGIT_SCALE
            * lax.dot_general(pair, texts, (((1,), (1,)), ((), ())), preferred_element_type=F32)
            + BIAS_LOGIT
        )
        row = lax.broadcasted_iota(jnp.int32, logits.shape, 0)
        col = lax.broadcasted_iota(jnp.int32, logits.shape, 1)
        gap = 8 * (col // ROWS) + 4 * (row // ROWS) + (s - j)
        match = (gap == 0) & (lax.rem(row, ROWS) == lax.rem(col, ROWS))
        weight = jax.nn.sigmoid(jnp.where(match, -logits, logits))
        weight = jnp.where(match, -weight, weight)
        weight = jnp.where((gap >= 0) & (gap <= 19), weight, 0.0)
        wgt[...] = weight.astype(BF16)
        for n in range(WIDTH // COLS):
            part = pl.ds(n * COLS, COLS)
            texts = txt[:, :, part].reshape(4 * ROWS, COLS)
            q = jnp.dot(wgt[...], texts, preferred_element_type=F32)
            q_sum[:, s, :, part] = q.reshape(2, ROWS, COLS)
            pair = img[:, s, :, part].reshape(2 * ROWS, COLS)
            p = lax.dot_general(wgt[...], pair, (((0,), (0,)), ((), ())), preferred_element_type=F32)
            p_sum[:, :, part] += p.reshape(4, ROWS, COLS)
        q_send[s] = q_sum[1 - k, s].astype(BF16)
        copy(q_send.at[s], q_recv.at[s], q_ssem.at[s], q_rsem.at[s], partner).start()

    def back_copy(d, h):
        return copy(p_send.at[d, thin(h)], p_recv.at[d, thin(h)], p_ssem.at[d, h], p_rsem.at[d, h], behind)

    def back_start(d, h):
        @pl.when(first)
        def _():
            copy(
                p_send.at[d, thin(h)], back_hold.at[d], p_ssem.at[d, h], back_rsem.at[d], at(0, relay_place(h))
            ).start()

        @pl.when(jnp.logical_not(first))
        def _():
            back_copy(d, h).start()

    def back_relay(d):
        return copy(
            back_hold.at[d], p_recv.at[d, thin(role)], back_ssem.at[d], p_rsem.at[d, role], prev_last
        )

    def back_relay_stage(d):
        @pl.when(relay & (j >= 5) if d == 2 else relay)
        def _():
            copy(back_hold.at[d], back_hold.at[d], back_ssem.at[d], back_rsem.at[d], prev_last).wait_recv()
            back_relay(d).start()

    def far_copy(t, h, receiver):
        s = spot(t)
        sem = {"near": near_rsem, "far": far_rsem}[receiver]
        dst = {"near": near_in, "far": far_in}[receiver]
        return copy(far_out.at[s, rows(h)], dst.at[s, rows(h)], far_ssem.at[s, h], sem.at[s, h], far)

    def near_copy(h):
        s = spot(0)
        return copy(near_out.at[rows(h)], far_in.at[s, rows(h)], near_ssem.at[h], far_rsem.at[s, h], near)

    def near_arrival(t, h):
        s = spot(t)
        copy(far_out.at[s, rows(h)], near_in.at[s, rows(h)], far_ssem.at[s, h], near_rsem.at[s, h], far).wait_recv()

    def far_arrival(t, h):
        s = spot(t)
        copy(far_out.at[s, rows(h)], far_in.at[s, rows(h)], far_ssem.at[s, h], far_rsem.at[s, h], far).wait_recv()

    @pl.when(j >= 5)
    def _():
        p_send[2] = p_sum[3].astype(BF16)
        for h in range(SLICES):
            back_start(2, h)

    @pl.loop(0, 4)
    def _(s):
        copy(q_send.at[s], q_recv.at[s], q_ssem.at[s], q_rsem.at[s], partner).wait_recv()

    for u in range(3):
        for h in range(CHUNKS):
            r = rows(h)

            @pl.when(edge)
            def _():
                t = spot(3 - u)
                far_out[t, r] = (q_sum[k, t, r] + q_recv[t, r].astype(F32)).astype(BF16)
                far_copy(3 - u, h, "near").start()

            if u < 2:
                @pl.when(middle)
                def _():
                    t = spot(3 - u)
                    near_arrival(3 - u, h)
                    total = q_sum[k, t, r] + q_recv[t, r].astype(F32) + near_in[t, r].astype(F32)
                    far_out[t, r] = total.astype(BF16)
                    far_copy(3 - u, h, "far").start()

            if u == 1:
                @pl.when(middle)
                def _():
                    t = spot(0)
                    far_arrival(0, h)
                    total = q_sum[k, t, r] + q_recv[t, r].astype(F32) + far_in[t, r].astype(F32)
                    near_out[r] = total.astype(BF16)
                    near_copy(h).start()

        back_relay_stage(2 - u)
        if u < 2:
            for h in range(SLICES):
                r = thin(h)
                if u == 0:
                    @pl.when(j >= 5)
                    def _():
                        back_copy(2, h).wait_recv()
                        p_send[1, r] = (p_sum[2, r] + p_recv[2, r].astype(F32)).astype(BF16)
                        back_start(1, h)

                    @pl.when(j < 5)
                    def _():
                        p_send[1, r] = p_sum[2, r].astype(BF16)
                        back_start(1, h)
                else:
                    back_copy(1, h).wait_recv()
                    p_send[0, r] = (p_sum[1, r] + p_recv[1, r].astype(F32)).astype(BF16)
                    back_start(0, h)

    for h in range(SLICES):
        back_copy(0, h).wait_recv()
    text_out[...] = undo(p_sum[0] + p_recv[0].astype(F32), text_ref)

    @pl.when(edge)
    def _():
        for h in range(CHUNKS):
            far_arrival(0, h)
        total = q_sum[k, z] + q_recv[z].astype(F32) + far_in[z].astype(F32)
        image_out[...] = undo(total, image_ref)

    @pl.when(middle)
    def _():
        for h in range(CHUNKS):
            near_arrival(1, h)
            far_arrival(1, h)
        total = q_sum[k, z] + q_recv[z].astype(F32) + near_in[z].astype(F32) + far_in[z].astype(F32)
        image_out[...] = undo(total, image_ref)

    for d in range(3):
        @pl.when(relay & (j >= 5) if d == 2 else relay)
        def _():
            text_relay(d).wait_send()
            back_relay(d).wait_send()

        @pl.when(j >= (5 if d == 2 else 0))
        def _():
            for h in range(SLICES):
                text_copy(d, h).wait_send()
                back_copy(d, h).wait_send()

    for h in range(CHUNKS):
        for t in range(4):
            image_copy(t, h, img_psem, partner).wait_send()

        @pl.when(edge)
        def _():
            image_copy(0, h, img_fsem, far).wait_send()
            for t in (1, 2, 3):
                far_copy(t, h, "near").wait_send()

        @pl.when(middle)
        def _():
            for t in (0, 1):
                image_copy(t, h, img_fsem, far).wait_send()
            for t in (1, 2, 3):
                image_copy(t, h, img_nsem, near).wait_send()
            for t in (2, 3):
                far_copy(t, h, "far").wait_send()
            near_copy(h).wait_send()

    @pl.loop(0, 4)
    def _(s):
        copy(q_send.at[s], q_recv.at[s], q_ssem.at[s], q_rsem.at[s], partner).wait_send()


def solution(mesh):
    blocks = mesh.shape["blk"]
    dma = pltpu.SemaphoreType.DMA
    block = (ROWS, WIDTH)

    def per_device(image_embeds, text_embeds):
        out = jax.ShapeDtypeStruct(block, BF16)
        vmem = pl.BlockSpec(memory_space=pltpu.VMEM)
        return pl.pallas_call(
            lambda *refs: kernel(blocks, *refs),
            out_shape=(out, out),
            in_specs=[vmem, vmem],
            out_specs=(vmem, vmem),
            scratch_shapes=[
                pltpu.VMEM((2, 4) + block, BF16),
                pltpu.VMEM((4,) + block, BF16),
                pltpu.VMEM((2 * ROWS, 4 * ROWS), BF16),
                pltpu.VMEM((2, 4) + block, F32),
                pltpu.VMEM((4,) + block, F32),
                pltpu.VMEM((4,) + block, BF16),
                pltpu.VMEM((4,) + block, BF16),
                pltpu.VMEM((4,) + block, BF16),
                pltpu.VMEM(block, BF16),
                pltpu.VMEM((4,) + block, BF16),
                pltpu.VMEM((4,) + block, BF16),
                pltpu.VMEM((3,) + block, BF16),
                pltpu.VMEM((3,) + block, BF16),
                pltpu.VMEM((3, THIN, WIDTH), BF16),
                pltpu.VMEM((3, THIN, WIDTH), BF16),
                dma((3, SLICES)),
                dma((3, SLICES)),
                dma((4, CHUNKS)),
                dma((4, CHUNKS)),
                dma((4, CHUNKS)),
                dma((2, 4, CHUNKS)),
                dma((4,)),
                dma((4,)),
                dma((4, CHUNKS)),
                dma((CHUNKS,)),
                dma((4, CHUNKS)),
                dma((4, CHUNKS)),
                dma((3, SLICES)),
                dma((3, SLICES)),
                dma((3,)),
                dma((3,)),
                dma((3,)),
                dma((3,)),
            ],
            compiler_params=pltpu.CompilerParams(
                collective_id=0, has_side_effects=True, vmem_limit_bytes=56 * 1024 * 1024
            ),
            name="pair_window",
        )(image_embeds, text_embeds)

    spec = P(("blk", "grp"), None)
    return jax.shard_map(
        per_device, mesh=mesh, in_specs=(spec, spec), out_specs=(spec, spec), check_vma=False
    )
```

```python
import jax
import jax.numpy as jnp
from jax import lax
from jax.experimental import pallas as pl
from jax.experimental.pallas import tpu as pltpu
from jax.sharding import PartitionSpec as P

MESH = pl.DeviceIdType.MESH
LOGIT_SCALE = 10.0
BIAS_LOGIT = -2.0
EPSILON = 1e-06
ROWS = 128
WIDTH = 1152
CHUNKS = 2
PIECE = ROWS // CHUNKS
SLICES = 4
THIN = ROWS // SLICES
RELAYS = ((24, 7, 1, 30), (23, 8, 15, 6))
COLS = 384
F32 = jnp.float32
BF16 = jnp.bfloat16


def unit_and_inverse(ref):
    wide = ref[...].astype(F32)
    length = jnp.sqrt(jnp.sum(wide * wide, axis=-1, keepdims=True) + EPSILON)
    inverse = 1.0 / length
    return wide * inverse, inverse


def undo(total, ref):
    unit, inverse = unit_and_inverse(ref)
    grad = LOGIT_SCALE * total
    inner = jnp.sum(unit * grad, axis=-1, keepdims=True)
    return ((grad - unit * inner) * inverse).astype(BF16)


def kernel(
    blocks,
    image_ref, text_ref, image_out, text_out,
    img, txt, wgt, q_sum, p_sum,
    q_send, q_recv, far_out, near_out, near_in, far_in, p_send, p_recv,
    fwd_hold, back_hold,
    txt_ssem, txt_rsem, img_fsem, img_nsem, img_psem, img_rsem,
    q_ssem, q_rsem, far_ssem, near_ssem, near_rsem, far_rsem, p_ssem, p_rsem,
    fwd_ssem, fwd_rsem, back_ssem, back_rsem,
):
    blk = lax.axis_index("blk")
    z = lax.axis_index("grp")
    k = lax.rem(blk, 2)
    j = 4 * k + z
    high = z // 2
    sign = 1 - 2 * high
    middle = (z == 1) | (z == 2)
    edge = (z == 0) | (z == 3)

    def spot(t):
        return 3 * high + sign * t

    column = blk // 2
    third = column // 32
    place = lax.rem(column, 32)
    first = place == 0
    last = place == 31

    def relay_place(h):
        return RELAYS[0][h] + k * (RELAYS[1][h] - RELAYS[0][h])

    def at(hop, where):
        return (2 * (32 * lax.rem(third + hop, blocks // 64) + where) + k, z)

    role, relay = 0, False
    for h in range(SLICES):
        match = place == relay_place(h)
        role = role + jnp.where(match, h, 0)
        relay = relay | match
    next_first, own_first = at(1, 0), at(0, 0)
    prev_last, own_last = at(blocks // 64 - 1, 31), at(0, 31)

    partner = (blk + 1 - 2 * k, z)
    ahead = (lax.rem(blk + 2, blocks), z)
    behind = (lax.rem(blk + blocks - 2, blocks), z)
    far = (blk, z + sign)
    near = (blk, z - sign)

    def copy(src, dst, ssem, rsem, device):
        return pltpu.make_async_remote_copy(
            src_ref=src, dst_ref=dst, send_sem=ssem, recv_sem=rsem, device_id=device, device_id_type=MESH
        )

    def rows(h):
        return pl.ds(h * PIECE, PIECE)

    def thin(h):
        return pl.ds(pl.multiple_of(h * THIN, THIN), THIN)

    barrier = pltpu.get_barrier_semaphore()

    def greet(condition, devices):
        @pl.when(condition)
        def _():
            for device in devices:
                pl.semaphore_signal(barrier, inc=1, device_id=device, device_id_type=MESH)

    greet(relay, (own_last, own_first))
    greet(first, [at(blocks // 64 - 1, relay_place(h)) for h in range(SLICES)])
    greet(last, [at(1, relay_place(h)) for h in range(SLICES)])
    for device in (partner, far):
        pl.semaphore_signal(barrier, inc=1, device_id=device, device_id_type=MESH)
    greet(middle, (near,))
    greet(jnp.logical_not(first), (behind,))
    greet(jnp.logical_not(last), (ahead,))

    unit, _ = unit_and_inverse(image_ref)
    img[k, z] = unit.astype(BF16)
    unit, _ = unit_and_inverse(text_ref)
    txt[0] = unit.astype(BF16)

    greeted = 4 + z * (3 - z) // 2 + jnp.where(relay, 2, 0) + jnp.where(first | last, SLICES - 1, 0)
    pl.semaphore_wait(barrier, greeted)

    def image_copy(t, h, ssem, device):
        s = spot(t)
        ref = img.at[k, s, rows(h)]
        return copy(ref, ref, ssem.at[t, h], img_rsem.at[k, s, h], device)

    def image_arrival(kk, s, h):
        ref = img.at[kk, s, rows(h)]
        copy(ref, ref, img_psem.at[0, h], img_rsem.at[kk, s, h], partner).wait_recv()

    def text_copy(d, h):
        return copy(
            txt.at[d, thin(h)], txt.at[d + 1, thin(h)], txt_ssem.at[d, h], txt_rsem.at[d, h], ahead
        )

    def text_start(d, h):
        @pl.when(last)
        def _():
            copy(
                txt.at[d, thin(h)], fwd_hold.at[d], txt_ssem.at[d, h], fwd_rsem.at[d], at(0, relay_place(h))
            ).start()

        @pl.when(jnp.logical_not(last))
        def _():
            text_copy(d, h).start()

    def text_relay(d):
        return copy(
            fwd_hold.at[d], txt.at[d + 1, thin(role)], fwd_ssem.at[d], txt_rsem.at[d, role], next_first
        )

    def text_relay_stage(d):
        @pl.when(relay & (j >= 5) if d == 2 else relay)
        def _():
            copy(fwd_hold.at[d], fwd_hold.at[d], fwd_ssem.at[d], fwd_rsem.at[d], next_first).wait_recv()
            text_relay(d).start()

    for h in range(SLICES):
        text_start(0, h)

    def back_copy(d, h):
        return copy(p_send.at[d, thin(h)], p_recv.at[d, thin(h)], p_ssem.at[d, h], p_rsem.at[d, h], behind)

    def back_start(d, h):
        @pl.when(first)
        def _():
            copy(
                p_send.at[d, thin(h)], back_hold.at[d], p_ssem.at[d, h], back_rsem.at[d], at(0, relay_place(h))
            ).start()

        @pl.when(jnp.logical_not(first))
        def _():
            back_copy(d, h).start()

    def back_relay(d):
        return copy(
            back_hold.at[d], p_recv.at[d, thin(role)], back_ssem.at[d], p_rsem.at[d, role], prev_last
        )

    def back_relay_stage(d):
        copy(back_hold.at[d], back_hold.at[d], back_ssem.at[d], back_rsem.at[d], prev_last).wait_recv()
        back_relay(d).start()

    def far_copy(t, h, receiver):
        s = spot(t)
        sem = {"near": near_rsem, "far": far_rsem}[receiver]
        dst = {"near": near_in, "far": far_in}[receiver]
        return copy(far_out.at[s, rows(h)], dst.at[s, rows(h)], far_ssem.at[s, h], sem.at[s, h], far)

    def near_copy(h):
        s = spot(0)
        return copy(near_out.at[rows(h)], far_in.at[s, rows(h)], near_ssem.at[h], far_rsem.at[s, h], near)

    def near_arrival(t, h):
        s = spot(t)
        copy(far_out.at[s, rows(h)], near_in.at[s, rows(h)], far_ssem.at[s, h], near_rsem.at[s, h], far).wait_recv()

    def far_arrival(t, h):
        s = spot(t)
        copy(far_out.at[s, rows(h)], far_in.at[s, rows(h)], far_ssem.at[s, h], far_rsem.at[s, h], far).wait_recv()

    def sum_arrival(t):
        s = spot(t)
        copy(q_send.at[s], q_recv.at[s], q_ssem.at[s], q_rsem.at[s], partner).wait_recv()

    def own_part(s, r):
        return q_sum[k, s, r] + q_recv[s, r].astype(F32)

    def far_start(t):
        sum_arrival(t)
        s = spot(t)
        for h in range(CHUNKS):
            r = rows(h)
            far_out[s, r] = own_part(s, r).astype(BF16)
            far_copy(t, h, "near").start()

    def far_pass(t):
        sum_arrival(t)
        s = spot(t)
        for h in range(CHUNKS):
            r = rows(h)
            near_arrival(t, h)
            far_out[s, r] = (own_part(s, r) + near_in[s, r].astype(F32)).astype(BF16)
            far_copy(t, h, "far").start()

    def near_pass():
        sum_arrival(0)
        s = spot(0)
        for h in range(CHUNKS):
            r = rows(h)
            far_arrival(0, h)
            near_out[r] = (own_part(s, r) + far_in[s, r].astype(F32)).astype(BF16)
            near_copy(h).start()

    def back_begin(d):
        for h in range(SLICES):
            r = thin(h)
            p_send[d - 1, r] = p_sum[d, r].astype(BF16)
            back_start(d - 1, h)

    def back_pass(d):
        for h in range(SLICES):
            r = thin(h)
            back_copy(d, h).wait_recv()
            p_send[d - 1, r] = (p_sum[d, r] + p_recv[d, r].astype(F32)).astype(BF16)
            back_start(d - 1, h)

    def image_first(h):
        @pl.when(edge)
        def _():
            image_copy(0, h, img_fsem, far).start()
            image_copy(0, h, img_psem, partner).start()

        @pl.when(middle)
        def _():
            image_copy(1, h, img_fsem, far).start()
            image_copy(1, h, img_nsem, near).start()
            image_copy(1, h, img_psem, partner).start()

    def image_stage(u):
        for h in range(CHUNKS):
            @pl.when(edge)
            def _():
                image_arrival(k, spot(u + 1), h)
                image_copy(u + 1, h, img_psem, partner).start()

            @pl.when(middle)
            def _():
                if u == 0:
                    image_arrival(k, spot(0), h)
                    image_copy(0, h, img_fsem, far).start()
                    image_copy(0, h, img_psem, partner).start()
                else:
                    image_arrival(k, spot(u + 1), h)
                    image_copy(u + 1, h, img_nsem, near).start()
                    image_copy(u + 1, h, img_psem, partner).start()

    def text_stage(u):
        for h in range(SLICES):
            text_copy(u, h).wait_recv()
            if u == 0:
                text_start(1, h)
            elif u == 1:
                @pl.when(j >= 5)
                def _():
                    text_start(2, h)

    def weights(logits, gap):
        logits = LOGIT_SCALE * logits + BIAS_LOGIT
        row = lax.broadcasted_iota(jnp.int32, logits.shape, 0)
        col = lax.broadcasted_iota(jnp.int32, logits.shape, 1)
        gap = gap + 8 * (col // ROWS) + 4 * (row // ROWS)
        match = (gap == 0) & (lax.rem(row, ROWS) == lax.rem(col, ROWS))
        weight = jax.nn.sigmoid(jnp.where(match, -logits, logits))
        weight = jnp.where(match, -weight, weight)
        return jnp.where((gap >= 0) & (gap <= 19), weight, 0.0).astype(BF16)

    NT = (((1,), (1,)), ((), ()))
    TN = (((0,), (0,)), ((), ()))

    def products(t):
        s = spot(t)
        for h in range(CHUNKS):
            image_arrival(1 - k, s, h)
        pair = img[:, s].reshape(2 * ROWS, WIDTH)
        texts = txt[0:3].reshape(3 * ROWS, WIDTH)
        wgt[...] = weights(lax.dot_general(pair, texts, NT, preferred_element_type=F32), s - j)
        for n in range(WIDTH // COLS):
            part = pl.ds(n * COLS, COLS)
            texts = txt[0:3, :, part].reshape(3 * ROWS, COLS)
            q = jnp.dot(wgt[...], texts, preferred_element_type=F32)
            q_sum[:, s, :, part] = q.reshape(2, ROWS, COLS)
            pair = img[:, s, :, part].reshape(2 * ROWS, COLS)
            p = lax.dot_general(wgt[...], pair, TN, preferred_element_type=F32)
            p_sum[0:3, :, part] += p.reshape(3, ROWS, COLS)

        @pl.when(j >= 5)
        def _():
            old = weights(lax.dot_general(img[0, s], txt[3], NT, preferred_element_type=F32), 24 + s - j)
            q_sum[0, s] += jnp.dot(old, txt[3], preferred_element_type=F32)
            p_sum[3] += lax.dot_general(old, img[0, s], TN, preferred_element_type=F32)

        q_send[s] = q_sum[1 - k, s].astype(BF16)
        copy(q_send.at[s], q_recv.at[s], q_ssem.at[s], q_rsem.at[s], partner).start()

    image_first(0)
    text_relay_stage(0)
    image_first(1)
    p_sum[...] = jnp.zeros_like(p_sum)
    for u in range(2):
        if u > 0:
            text_relay_stage(u)
        image_stage(u)
        text_stage(u)

    @pl.when(middle)
    def _():
        for h in range(CHUNKS):
            image_arrival(k, spot(3), h)
            image_copy(3, h, img_nsem, near).start()
            image_copy(3, h, img_psem, partner).start()

    text_relay_stage(2)

    @pl.when(j >= 5)
    def _():
        text_stage(2)

    @pl.loop(0, 4)
    def _(i):
        t = lax.rem(6 - i, 4)

        @pl.when(edge & (i == 3))
        def _():
            for h in range(CHUNKS):
                image_arrival(k, spot(3), h)
                image_copy(3, h, img_psem, partner).start()
            far_start(2)

        products(t)

    late = j >= 5
    soon = j < 5

    def when(condition, run, *args):
        @pl.when(condition)
        def _():
            run(*args)

    slow = last | (late & (place == 30))
    when(late, back_begin, 3)
    when(soon, back_begin, 2)
    when(edge, far_start, 3)
    when(late & jnp.logical_not(last), back_pass, 2)
    when(middle, far_pass, 2)
    when(relay & late, back_relay_stage, 2)
    when(relay & soon, back_relay_stage, 1)
    when(edge, far_start, 1)
    when(jnp.logical_not(slow), back_pass, 1)
    when(middle, far_pass, 3)
    when(relay & late, back_relay_stage, 1)
    when(relay & soon, back_relay_stage, 0)
    when(middle, near_pass)
    when(late & last, back_pass, 2)
    when(slow, back_pass, 1)
    when(relay & late, back_relay_stage, 0)
    when(edge, sum_arrival, 0)
    when(middle, sum_arrival, 1)

    for h in range(SLICES):
        back_copy(0, h).wait_recv()
    text_out[...] = undo(p_sum[0] + p_recv[0].astype(F32), text_ref)

    @pl.when(edge)
    def _():
        for h in range(CHUNKS):
            far_arrival(0, h)
        total = q_sum[k, z] + q_recv[z].astype(F32) + far_in[z].astype(F32)
        image_out[...] = undo(total, image_ref)

    @pl.when(middle)
    def _():
        for h in range(CHUNKS):
            near_arrival(1, h)
            far_arrival(1, h)
        total = q_sum[k, z] + q_recv[z].astype(F32) + near_in[z].astype(F32) + far_in[z].astype(F32)
        image_out[...] = undo(total, image_ref)

    for d in range(3):
        @pl.when(relay & (j >= 5) if d == 2 else relay)
        def _():
            text_relay(d).wait_send()
            back_relay(d).wait_send()

        @pl.when(j >= (5 if d == 2 else 0))
        def _():
            for h in range(SLICES):
                text_copy(d, h).wait_send()
                back_copy(d, h).wait_send()

    for h in range(CHUNKS):
        for t in range(4):
            image_copy(t, h, img_psem, partner).wait_send()

        @pl.when(edge)
        def _():
            image_copy(0, h, img_fsem, far).wait_send()
            for t in (1, 2, 3):
                far_copy(t, h, "near").wait_send()

        @pl.when(middle)
        def _():
            for t in (0, 1):
                image_copy(t, h, img_fsem, far).wait_send()
            for t in (1, 2, 3):
                image_copy(t, h, img_nsem, near).wait_send()
            for t in (2, 3):
                far_copy(t, h, "far").wait_send()
            near_copy(h).wait_send()

    @pl.loop(0, 4)
    def _(s):
        copy(q_send.at[s], q_recv.at[s], q_ssem.at[s], q_rsem.at[s], partner).wait_send()


def solution(mesh):
    blocks = mesh.shape["blk"]
    dma = pltpu.SemaphoreType.DMA
    block = (ROWS, WIDTH)

    def per_device(image_embeds, text_embeds):
        out = jax.ShapeDtypeStruct(block, BF16)
        vmem = pl.BlockSpec(memory_space=pltpu.VMEM)
        return pl.pallas_call(
            lambda *refs: kernel(blocks, *refs),
            out_shape=(out, out),
            in_specs=[vmem, vmem],
            out_specs=(vmem, vmem),
            scratch_shapes=[
                pltpu.VMEM((2, 4) + block, BF16),
                pltpu.VMEM((4,) + block, BF16),
                pltpu.VMEM((2 * ROWS, 3 * ROWS), BF16),
                pltpu.VMEM((2, 4) + block, F32),
                pltpu.VMEM((4,) + block, F32),
                pltpu.VMEM((4,) + block, BF16),
                pltpu.VMEM((4,) + block, BF16),
                pltpu.VMEM((4,) + block, BF16),
                pltpu.VMEM(block, BF16),
                pltpu.VMEM((4,) + block, BF16),
                pltpu.VMEM((4,) + block, BF16),
                pltpu.VMEM((3,) + block, BF16),
                pltpu.VMEM((3,) + block, BF16),
                pltpu.VMEM((3, THIN, WIDTH), BF16),
                pltpu.VMEM((3, THIN, WIDTH), BF16),
                dma((3, SLICES)),
                dma((3, SLICES)),
                dma((4, CHUNKS)),
                dma((4, CHUNKS)),
                dma((4, CHUNKS)),
                dma((2, 4, CHUNKS)),
                dma((4,)),
                dma((4,)),
                dma((4, CHUNKS)),
                dma((CHUNKS,)),
                dma((4, CHUNKS)),
                dma((4, CHUNKS)),
                dma((3, SLICES)),
                dma((3, SLICES)),
                dma((3,)),
                dma((3,)),
                dma((3,)),
                dma((3,)),
            ],
            compiler_params=pltpu.CompilerParams(
                collective_id=0, has_side_effects=True, vmem_limit_bytes=56 * 1024 * 1024
            ),
            name="pair_window",
        )(image_embeds, text_embeds)

    spec = P(("blk", "grp"), None)
    return jax.shard_map(
        per_device, mesh=mesh, in_specs=(spec, spec), out_specs=(spec, spec), check_vma=False
    )
```

```python
import jax
import jax.numpy as jnp
from jax import lax
from jax.experimental import pallas as pl
from jax.experimental.pallas import tpu as pltpu
from jax.sharding import PartitionSpec as P

MESH = pl.DeviceIdType.MESH
LOGIT_SCALE = 10.0
BIAS_LOGIT = -2.0
EPSILON = 1e-06
ROWS = 128
WIDTH = 1152
CHUNKS = 2
PIECE = ROWS // CHUNKS
SLICES = 8
THIN = ROWS // SLICES
RELAYS = ((26, 14, 17, 30, 1, 16, 7, 24), (9, 5, 22, 8, 6, 25, 15, 23))
COLS = 384
F32 = jnp.float32
BF16 = jnp.bfloat16


def unit_and_inverse(ref):
    wide = ref[...].astype(F32)
    length = jnp.sqrt(jnp.sum(wide * wide, axis=-1, keepdims=True) + EPSILON)
    inverse = 1.0 / length
    return wide * inverse, inverse


def undo(total, ref):
    unit, inverse = unit_and_inverse(ref)
    grad = LOGIT_SCALE * total
    inner = jnp.sum(unit * grad, axis=-1, keepdims=True)
    return ((grad - unit * inner) * inverse).astype(BF16)


def kernel(
    blocks,
    image_ref, text_ref, image_out, text_out,
    img, txt, wgt, q_sum, p_sum,
    q_send, q_recv, far_out, near_out, near_in, far_in, p_send, p_recv,
    fwd_hold, back_hold,
    txt_ssem, txt_rsem, img_fsem, img_nsem, img_psem, img_rsem,
    q_ssem, q_rsem, far_ssem, near_ssem, near_rsem, far_rsem, p_ssem, p_rsem,
    fwd_ssem, fwd_rsem, back_ssem, back_rsem,
):
    blk = lax.axis_index("blk")
    z = lax.axis_index("grp")
    k = lax.rem(blk, 2)
    j = 4 * k + z
    high = z // 2
    sign = 1 - 2 * high
    middle = (z == 1) | (z == 2)
    edge = (z == 0) | (z == 3)

    def spot(t):
        return 3 * high + sign * t

    column = blk // 2
    third = column // 32
    place = lax.rem(column, 32)
    first = place == 0
    last = place == 31

    def relay_place(h):
        return RELAYS[0][h] + k * (RELAYS[1][h] - RELAYS[0][h])

    def at(hop, where):
        return (2 * (32 * lax.rem(third + hop, blocks // 64) + where) + k, z)

    role, relay = 0, False
    for h in range(SLICES):
        match = place == relay_place(h)
        role = role + jnp.where(match, h, 0)
        relay = relay | match
    next_first, own_first = at(1, 0), at(0, 0)
    prev_last, own_last = at(blocks // 64 - 1, 31), at(0, 31)

    partner = (blk + 1 - 2 * k, z)
    ahead = (lax.rem(blk + 2, blocks), z)
    behind = (lax.rem(blk + blocks - 2, blocks), z)
    far = (blk, z + sign)
    near = (blk, z - sign)

    def copy(src, dst, ssem, rsem, device):
        return pltpu.make_async_remote_copy(
            src_ref=src, dst_ref=dst, send_sem=ssem, recv_sem=rsem, device_id=device, device_id_type=MESH
        )

    def rows(h):
        return pl.ds(h * PIECE, PIECE)

    def thin(h):
        return pl.ds(pl.multiple_of(h * THIN, THIN), THIN)

    barrier = pltpu.get_barrier_semaphore()

    def greet(condition, devices):
        @pl.when(condition)
        def _():
            for device in devices:
                pl.semaphore_signal(barrier, inc=1, device_id=device, device_id_type=MESH)

    greet(relay, (own_last, own_first))
    greet(first, [at(blocks // 64 - 1, relay_place(h)) for h in range(SLICES)])
    greet(last, [at(1, relay_place(h)) for h in range(SLICES)])
    for device in (partner, far):
        pl.semaphore_signal(barrier, inc=1, device_id=device, device_id_type=MESH)
    greet(middle, (near,))
    greet(jnp.logical_not(first), (behind,))
    greet(jnp.logical_not(last), (ahead,))

    unit, _ = unit_and_inverse(image_ref)
    img[k, z] = unit.astype(BF16)
    unit, _ = unit_and_inverse(text_ref)
    txt[0] = unit.astype(BF16)

    greeted = 4 + z * (3 - z) // 2 + jnp.where(relay, 2, 0) + jnp.where(first | last, SLICES - 1, 0)
    pl.semaphore_wait(barrier, greeted)

    def image_copy(t, h, ssem, device):
        s = spot(t)
        ref = img.at[k, s, rows(h)]
        return copy(ref, ref, ssem.at[t, h], img_rsem.at[k, s, h], device)

    def image_arrival(kk, s, h):
        ref = img.at[kk, s, rows(h)]
        copy(ref, ref, img_psem.at[0, h], img_rsem.at[kk, s, h], partner).wait_recv()

    def text_copy(d, h):
        return copy(
            txt.at[d, thin(h)], txt.at[d + 1, thin(h)], txt_ssem.at[d, h], txt_rsem.at[d, h], ahead
        )

    def text_start(d, h):
        @pl.when(last)
        def _():
            copy(
                txt.at[d, thin(h)], fwd_hold.at[d], txt_ssem.at[d, h], fwd_rsem.at[d], at(0, relay_place(h))
            ).start()

        @pl.when(jnp.logical_not(last))
        def _():
            text_copy(d, h).start()

    def text_relay(d):
        return copy(
            fwd_hold.at[d], txt.at[d + 1, thin(role)], fwd_ssem.at[d], txt_rsem.at[d, role], next_first
        )

    def text_relay_stage(d):
        @pl.when(relay & (j >= 5) if d == 2 else relay)
        def _():
            copy(fwd_hold.at[d], fwd_hold.at[d], fwd_ssem.at[d], fwd_rsem.at[d], next_first).wait_recv()
            text_relay(d).start()

    for h in range(SLICES):
        text_start(0, h)

    def back_copy(d, h):
        return copy(p_send.at[d, thin(h)], p_recv.at[d, thin(h)], p_ssem.at[d, h], p_rsem.at[d, h], behind)

    def back_start(d, h):
        @pl.when(first)
        def _():
            copy(
                p_send.at[d, thin(h)], back_hold.at[d], p_ssem.at[d, h], back_rsem.at[d], at(0, relay_place(h))
            ).start()

        @pl.when(jnp.logical_not(first))
        def _():
            back_copy(d, h).start()

    def back_relay(d):
        return copy(
            back_hold.at[d], p_recv.at[d, thin(role)], back_ssem.at[d], p_rsem.at[d, role], prev_last
        )

    def back_relay_stage(d):
        copy(back_hold.at[d], back_hold.at[d], back_ssem.at[d], back_rsem.at[d], prev_last).wait_recv()
        back_relay(d).start()

    def far_copy(t, h, receiver):
        s = spot(t)
        sem = {"near": near_rsem, "far": far_rsem}[receiver]
        dst = {"near": near_in, "far": far_in}[receiver]
        return copy(far_out.at[s, rows(h)], dst.at[s, rows(h)], far_ssem.at[s, h], sem.at[s, h], far)

    def near_copy(h):
        s = spot(0)
        return copy(near_out.at[rows(h)], far_in.at[s, rows(h)], near_ssem.at[h], far_rsem.at[s, h], near)

    def near_arrival(t, h):
        s = spot(t)
        copy(far_out.at[s, rows(h)], near_in.at[s, rows(h)], far_ssem.at[s, h], near_rsem.at[s, h], far).wait_recv()

    def far_arrival(t, h):
        s = spot(t)
        copy(far_out.at[s, rows(h)], far_in.at[s, rows(h)], far_ssem.at[s, h], far_rsem.at[s, h], far).wait_recv()

    def sum_arrival(t):
        s = spot(t)
        copy(q_send.at[s], q_recv.at[s], q_ssem.at[s], q_rsem.at[s], partner).wait_recv()

    def own_part(s, r):
        return q_sum[k, s, r] + q_recv[s, r].astype(F32)

    def far_start(t):
        sum_arrival(t)
        s = spot(t)
        for h in range(CHUNKS):
            r = rows(h)
            far_out[s, r] = own_part(s, r).astype(BF16)
            far_copy(t, h, "near").start()

    def far_pass(t):
        sum_arrival(t)
        s = spot(t)
        for h in range(CHUNKS):
            r = rows(h)
            near_arrival(t, h)
            far_out[s, r] = (own_part(s, r) + near_in[s, r].astype(F32)).astype(BF16)
            far_copy(t, h, "far").start()

    def near_pass():
        sum_arrival(0)
        s = spot(0)
        for h in range(CHUNKS):
            r = rows(h)
            far_arrival(0, h)
            near_out[r] = (own_part(s, r) + far_in[s, r].astype(F32)).astype(BF16)
            near_copy(h).start()

    def back_begin(d):
        for h in range(SLICES):
            r = thin(h)
            p_send[d - 1, r] = p_sum[d, r].astype(BF16)
            back_start(d - 1, h)

    def back_pass(d):
        for h in range(SLICES):
            r = thin(h)
            back_copy(d, h).wait_recv()
            p_send[d - 1, r] = (p_sum[d, r] + p_recv[d, r].astype(F32)).astype(BF16)
            back_start(d - 1, h)

    def image_first(h):
        @pl.when(edge)
        def _():
            image_copy(0, h, img_fsem, far).start()
            image_copy(0, h, img_psem, partner).start()

        @pl.when(middle)
        def _():
            image_copy(1, h, img_fsem, far).start()
            image_copy(1, h, img_nsem, near).start()
            image_copy(1, h, img_psem, partner).start()

    def image_stage(u):
        for h in range(CHUNKS):
            @pl.when(edge)
            def _():
                image_arrival(k, spot(u + 1), h)
                image_copy(u + 1, h, img_psem, partner).start()

            @pl.when(middle)
            def _():
                if u == 0:
                    image_arrival(k, spot(0), h)
                    image_copy(0, h, img_fsem, far).start()
                    image_copy(0, h, img_psem, partner).start()
                else:
                    image_arrival(k, spot(u + 1), h)
                    image_copy(u + 1, h, img_nsem, near).start()
                    image_copy(u + 1, h, img_psem, partner).start()

    def text_stage(u):
        for h in range(SLICES):
            text_copy(u, h).wait_recv()
            if u == 0:
                text_start(1, h)
            elif u == 1:
                @pl.when(j >= 5)
                def _():
                    text_start(2, h)

    def weights(logits, gap):
        logits = LOGIT_SCALE * logits + BIAS_LOGIT
        row = lax.broadcasted_iota(jnp.int32, logits.shape, 0)
        col = lax.broadcasted_iota(jnp.int32, logits.shape, 1)
        gap = gap + 8 * (col // ROWS) + 4 * (row // ROWS)
        match = (gap == 0) & (lax.rem(row, ROWS) == lax.rem(col, ROWS))
        weight = jax.nn.sigmoid(jnp.where(match, -logits, logits))
        weight = jnp.where(match, -weight, weight)
        return jnp.where((gap >= 0) & (gap <= 19), weight, 0.0).astype(BF16)

    NT = (((1,), (1,)), ((), ()))
    TN = (((0,), (0,)), ((), ()))

    def products(t, first_text, texts):
        s = spot(t)
        part_w = wgt.at[:, pl.ds(0, texts * ROWS)]
        near_texts = pl.ds(first_text, texts)
        pair = img[:, s].reshape(2 * ROWS, WIDTH)
        block = txt[near_texts].reshape(texts * ROWS, WIDTH)
        logits = lax.dot_general(pair, block, NT, preferred_element_type=F32)
        part_w[...] = weights(logits, 8 * first_text + s - j)
        for n in range(WIDTH // COLS):
            part = pl.ds(n * COLS, COLS)
            block = txt[near_texts, :, part].reshape(texts * ROWS, COLS)
            q = jnp.dot(part_w[...], block, preferred_element_type=F32).reshape(2, ROWS, COLS)
            pair = img[:, s, :, part].reshape(2 * ROWS, COLS)
            p = lax.dot_general(part_w[...], pair, TN, preferred_element_type=F32)
            if first_text == 0:
                q_sum[:, s, :, part] = q
            else:
                q_sum[:, s, :, part] += q
            p_sum[near_texts, :, part] += p.reshape(texts, ROWS, COLS)

    def recent(t):
        s = spot(t)
        for h in range(CHUNKS):
            image_arrival(1 - k, s, h)
        products(t, 0, 2)

    def share(s):
        q_send[s] = q_sum[1 - k, s].astype(BF16)
        copy(q_send.at[s], q_recv.at[s], q_ssem.at[s], q_rsem.at[s], partner).start()

    def older(t):
        products(t, 2, 1)

        @pl.when((j < 5) | (spot(t) >= z))
        def _():
            share(spot(t))

    def oldest(start, stop):
        @pl.loop(start, stop)
        def _(s):
            old = weights(lax.dot_general(img[0, s], txt[3], NT, preferred_element_type=F32), 24 + s - j)
            q_sum[0, s] += jnp.dot(old, txt[3], preferred_element_type=F32)
            p_sum[3] += lax.dot_general(old, img[0, s], TN, preferred_element_type=F32)
            share(s)

    late = j >= 5
    soon = j < 5

    def when(condition, run, *args):
        @pl.when(condition)
        def _():
            run(*args)

    image_first(0)
    text_relay_stage(0)
    image_first(1)
    p_sum[...] = jnp.zeros_like(p_sum)
    image_stage(0)
    when(middle, image_stage, 1)
    when(middle & first, image_stage, 2)
    text_stage(0)

    @pl.loop(0, 2 + z * (3 - z) // 2)
    def _(i):
        recent(jnp.where(i < 2, 1 - i, 2))

    text_relay_stage(1)
    when(edge, image_stage, 1)
    when(middle & jnp.logical_not(first), image_stage, 2)
    text_stage(1)
    text_relay_stage(2)
    when(edge, recent, 2)

    @pl.loop(0, 3)
    def _(i):
        older(2 - i)

    when(edge, image_stage, 2)

    @pl.when(late & edge)
    def _():
        text_stage(2)
        oldest(1, 3)

    when(edge, far_start, 2)
    recent(3)
    older(3)

    @pl.when(late & middle)
    def _():
        text_stage(2)

    @pl.when(late)
    def _():
        oldest(0, jnp.where(middle, z, 1))


    slow = last | (late & (place == 30))
    when(late, back_begin, 3)
    when(soon, back_begin, 2)
    when(edge, far_start, 3)
    when(late & jnp.logical_not(last), back_pass, 2)
    when(middle, far_pass, 2)
    when(relay & late, back_relay_stage, 2)
    when(relay & soon, back_relay_stage, 1)
    hold = relay & (z == 3)
    when(edge & jnp.logical_not(hold), far_start, 1)
    when(jnp.logical_not(slow), back_pass, 1)
    when(middle, far_pass, 3)
    when(relay & late, back_relay_stage, 1)
    when(relay & soon, back_relay_stage, 0)
    when(hold, far_start, 1)
    when(middle, near_pass)
    when(late & last, back_pass, 2)
    when(slow, back_pass, 1)
    when(relay & late, back_relay_stage, 0)
    when(edge, sum_arrival, 0)
    when(middle, sum_arrival, 1)

    for h in range(SLICES):
        back_copy(0, h).wait_recv()
    text_out[...] = undo(p_sum[0] + p_recv[0].astype(F32), text_ref)

    @pl.when(edge)
    def _():
        for h in range(CHUNKS):
            far_arrival(0, h)
        total = q_sum[k, z] + q_recv[z].astype(F32) + far_in[z].astype(F32)
        image_out[...] = undo(total, image_ref)

    @pl.when(middle)
    def _():
        for h in range(CHUNKS):
            near_arrival(1, h)
            far_arrival(1, h)
        total = q_sum[k, z] + q_recv[z].astype(F32) + near_in[z].astype(F32) + far_in[z].astype(F32)
        image_out[...] = undo(total, image_ref)

    for d in range(3):
        @pl.when(relay & (j >= 5) if d == 2 else relay)
        def _():
            text_relay(d).wait_send()
            back_relay(d).wait_send()

        @pl.when(j >= (5 if d == 2 else 0))
        def _():
            for h in range(SLICES):
                text_copy(d, h).wait_send()
                back_copy(d, h).wait_send()

    for h in range(CHUNKS):
        for t in range(4):
            image_copy(t, h, img_psem, partner).wait_send()

        @pl.when(edge)
        def _():
            image_copy(0, h, img_fsem, far).wait_send()
            for t in (1, 2, 3):
                far_copy(t, h, "near").wait_send()

        @pl.when(middle)
        def _():
            for t in (0, 1):
                image_copy(t, h, img_fsem, far).wait_send()
            for t in (1, 2, 3):
                image_copy(t, h, img_nsem, near).wait_send()
            for t in (2, 3):
                far_copy(t, h, "far").wait_send()
            near_copy(h).wait_send()

    @pl.loop(0, 4)
    def _(s):
        copy(q_send.at[s], q_recv.at[s], q_ssem.at[s], q_rsem.at[s], partner).wait_send()


def solution(mesh):
    blocks = mesh.shape["blk"]
    dma = pltpu.SemaphoreType.DMA
    block = (ROWS, WIDTH)

    def per_device(image_embeds, text_embeds):
        out = jax.ShapeDtypeStruct(block, BF16)
        vmem = pl.BlockSpec(memory_space=pltpu.VMEM)
        return pl.pallas_call(
            lambda *refs: kernel(blocks, *refs),
            out_shape=(out, out),
            in_specs=[vmem, vmem],
            out_specs=(vmem, vmem),
            scratch_shapes=[
                pltpu.VMEM((2, 4) + block, BF16),
                pltpu.VMEM((4,) + block, BF16),
                pltpu.VMEM((2 * ROWS, 3 * ROWS), BF16),
                pltpu.VMEM((2, 4) + block, F32),
                pltpu.VMEM((4,) + block, F32),
                pltpu.VMEM((4,) + block, BF16),
                pltpu.VMEM((4,) + block, BF16),
                pltpu.VMEM((4,) + block, BF16),
                pltpu.VMEM(block, BF16),
                pltpu.VMEM((4,) + block, BF16),
                pltpu.VMEM((4,) + block, BF16),
                pltpu.VMEM((3,) + block, BF16),
                pltpu.VMEM((3,) + block, BF16),
                pltpu.VMEM((3, THIN, WIDTH), BF16),
                pltpu.VMEM((3, THIN, WIDTH), BF16),
                dma((3, SLICES)),
                dma((3, SLICES)),
                dma((4, CHUNKS)),
                dma((4, CHUNKS)),
                dma((4, CHUNKS)),
                dma((2, 4, CHUNKS)),
                dma((4,)),
                dma((4,)),
                dma((4, CHUNKS)),
                dma((CHUNKS,)),
                dma((4, CHUNKS)),
                dma((4, CHUNKS)),
                dma((3, SLICES)),
                dma((3, SLICES)),
                dma((3,)),
                dma((3,)),
                dma((3,)),
                dma((3,)),
            ],
            compiler_params=pltpu.CompilerParams(
                collective_id=0, has_side_effects=True, vmem_limit_bytes=56 * 1024 * 1024
            ),
            name="pair_window",
        )(image_embeds, text_embeds)

    spec = P(("blk", "grp"), None)
    return jax.shard_map(
        per_device, mesh=mesh, in_specs=(spec, spec), out_specs=(spec, spec), check_vma=False
    )
```

```python
import jax
import jax.numpy as jnp
from jax import lax
from jax.experimental import pallas as pl
from jax.experimental.pallas import tpu as pltpu
from jax.sharding import PartitionSpec as P

MESH = pl.DeviceIdType.MESH
LOGIT_SCALE = 10.0
BIAS_LOGIT = -2.0
EPSILON = 1e-06
ROWS = 128
WIDTH = 1152
CHUNKS = 4
PIECE = ROWS // CHUNKS
SLICES = 8
THIN = ROWS // SLICES
RELAYS = ((26, 14, 17, 29, 1, 16, 7, 24), (9, 5, 22, 8, 6, 25, 15, 23))
COLS = 384
F32 = jnp.float32
BF16 = jnp.bfloat16


def unit_and_inverse(ref):
    wide = ref[...].astype(F32)
    length = jnp.sqrt(jnp.sum(wide * wide, axis=-1, keepdims=True) + EPSILON)
    inverse = 1.0 / length
    return wide * inverse, inverse


def undo(total, ref):
    unit, inverse = unit_and_inverse(ref)
    grad = LOGIT_SCALE * total
    inner = jnp.sum(unit * grad, axis=-1, keepdims=True)
    return ((grad - unit * inner) * inverse).astype(BF16)


def kernel(
    blocks,
    image_in, text_in, image_out, text_out,
    image_ref, text_ref, in_sem,
    img, txt, wgt, q_sum, p_sum,
    q_send, q_recv, far_out, near_out, near_in, far_in, p_send, p_recv,
    fwd_hold, back_hold,
    txt_ssem, txt_rsem, img_fsem, img_nsem, img_psem, img_rsem,
    q_ssem, q_rsem, far_ssem, near_ssem, near_rsem, far_rsem, p_ssem, p_rsem,
    ante_ssem, fwd_ssem, fwd_rsem, back_ssem, back_rsem, fwd_ready, back_ready, lane_ready,
):
    blk = lax.axis_index("blk")
    z = lax.axis_index("grp")
    k = lax.rem(blk, 2)
    j = 4 * k + z
    high = z // 2
    sign = 1 - 2 * high
    middle = (z == 1) | (z == 2)
    edge = (z == 0) | (z == 3)

    def spot(t):
        return 3 * high + sign * t

    column = blk // 2
    third = column // 32
    place = lax.rem(column, 32)
    first = place == 0
    last = place == 31
    ante = place == 30

    def relay_place(h):
        return RELAYS[0][h] + k * (RELAYS[1][h] - RELAYS[0][h])

    def at(hop, where):
        return (2 * (32 * lax.rem(third + hop, blocks // 64) + where) + k, z)

    role, relay = 0, False
    for h in range(SLICES):
        match = place == relay_place(h)
        role = role + jnp.where(match, h, 0)
        relay = relay | match
    next_first, own_first = at(1, 0), at(0, 0)
    prev_last, own_last, own_ante = at(blocks // 64 - 1, 31), at(0, 31), at(0, 30)

    partner = (blk + 1 - 2 * k, z)
    ahead = (lax.rem(blk + 2, blocks), z)
    behind = (lax.rem(blk + blocks - 2, blocks), z)
    far = (blk, z + sign)
    near = (blk, z - sign)

    def when(condition, run, *args):
        @pl.when(condition)
        def _():
            run(*args)

    def copy(src, dst, ssem, rsem, device):
        return pltpu.make_async_remote_copy(
            src_ref=src, dst_ref=dst, send_sem=ssem, recv_sem=rsem, device_id=device, device_id_type=MESH
        )

    def rows(h):
        return pl.ds(h * PIECE, PIECE)

    def thin(h):
        return pl.ds(pl.multiple_of(h * THIN, THIN), THIN)

    image_load = pltpu.make_async_copy(image_in, image_ref, in_sem.at[0])
    text_load = pltpu.make_async_copy(text_in, text_ref, in_sem.at[1])
    image_load.start()
    text_load.start()

    barrier = pltpu.get_barrier_semaphore()

    def greet(condition, devices):
        @pl.when(condition)
        def _():
            for device in devices:
                pl.semaphore_signal(barrier, inc=1, device_id=device, device_id_type=MESH)

    thirds = blocks // 64
    early, final = third == 0, third == thirds - 1
    not_early, not_final = jnp.logical_not(early), jnp.logical_not(final)
    past_relays = [at(thirds - 1, relay_place(h)) for h in range(SLICES)]
    coming_relays = [at(1, relay_place(h)) for h in range(SLICES)]
    own_relays = [at(0, relay_place(h)) for h in range(SLICES)]
    greet(relay, (own_last, own_ante))
    greet(first, own_relays)
    greet(first & early, past_relays)
    greet(last & not_final, coming_relays)
    greet(relay & not_final, (next_first,))
    greet(relay & early, (prev_last,))
    for device in (partner, far):
        pl.semaphore_signal(barrier, inc=1, device_id=device, device_id_type=MESH)
    greet(middle, (near,))
    greet(jnp.logical_not(first), (behind,))
    greet(jnp.logical_not(last), (ahead,))

    image_load.wait()
    unit, _ = unit_and_inverse(image_ref)
    img[k, z] = unit.astype(BF16)
    text_load.wait()
    unit, _ = unit_and_inverse(text_ref)
    txt[0] = unit.astype(BF16)

    answer_first, answer_last = first & not_early, last & final
    greeted = 4 + z * (3 - z) // 2 + jnp.where(last, SLICES - 1, 0) - jnp.where(first, 1, 0)
    greeted = greeted + jnp.where(answer_first | answer_last | ante, SLICES, 0)
    greeted = greeted + jnp.where(relay & final, 1, 0) + jnp.where(relay & not_early, 1, 0) + jnp.where(relay, 1, 0)
    pl.semaphore_wait(barrier, greeted)

    when(relay, lambda: pl.semaphore_signal(lane_ready, inc=1, device_id=own_first, device_id_type=MESH))

    @pl.when(answer_first)
    def _():
        for device in past_relays:
            pl.semaphore_signal(fwd_ready, inc=1, device_id=device, device_id_type=MESH)

    @pl.when(answer_last)
    def _():
        for device in coming_relays:
            pl.semaphore_signal(back_ready, inc=1, device_id=device, device_id_type=MESH)

    def image_copy(t, h, ssem, device):
        s = spot(t)
        ref = img.at[k, s, rows(h)]
        return copy(ref, ref, ssem.at[t, h], img_rsem.at[k, s, h], device)

    def image_arrival(kk, s, h):
        ref = img.at[kk, s, rows(h)]
        copy(ref, ref, img_psem.at[0, h], img_rsem.at[kk, s, h], partner).wait_recv()

    def text_copy(d, h):
        return copy(
            txt.at[d, thin(h)], txt.at[d + 1, thin(h)], txt_ssem.at[d, h], txt_rsem.at[d, h], ahead
        )

    def relay_copy(d, hold, h, ssem):
        return copy(txt.at[d, thin(h)], fwd_hold.at[hold], ssem, fwd_rsem.at[hold], at(0, relay_place(h)))

    def ante_copy(d, h):
        return relay_copy(d, d + 1, h, ante_ssem.at[d, h])

    def text_start(d, h):
        if d == 1:
            @pl.when(ante & (j >= 5))
            def _():
                ante_copy(1, h).start()

        @pl.when(jnp.logical_not(last))
        def _():
            text_copy(d, h).start()

        if d == 0:
            @pl.when(last)
            def _():
                relay_copy(0, 0, h, txt_ssem.at[0, h]).start()

    def text_relay(d):
        return copy(
            fwd_hold.at[d], txt.at[d + 1, thin(role)], fwd_ssem.at[d], txt_rsem.at[d, role], next_first
        )

    def text_relay_stage(d):
        copy(fwd_hold.at[d], fwd_hold.at[d], fwd_ssem.at[d], fwd_rsem.at[d], next_first).wait_recv()
        text_relay(d).start()

    for h in range(SLICES):
        when(ante, lambda h=h: ante_copy(0, h).start())

    for h in range(SLICES):
        text_start(0, h)

    def back_copy(d, h):
        return copy(p_send.at[d, thin(h)], p_recv.at[d, thin(h)], p_ssem.at[d, h], p_rsem.at[d, h], behind)

    def back_start(d, h):
        @pl.when(first)
        def _():
            copy(
                p_send.at[d, thin(h)], back_hold.at[d], p_ssem.at[d, h], back_rsem.at[d], at(0, relay_place(h))
            ).start()

        @pl.when(jnp.logical_not(first))
        def _():
            back_copy(d, h).start()

    def back_relay(d):
        return copy(
            back_hold.at[d], p_recv.at[d, thin(role)], back_ssem.at[d], p_rsem.at[d, role], prev_last
        )

    def back_relay_stage(d):
        copy(back_hold.at[d], back_hold.at[d], back_ssem.at[d], back_rsem.at[d], prev_last).wait_recv()
        back_relay(d).start()

    def far_copy(t, h, receiver):
        s = spot(t)
        sem = {"near": near_rsem, "far": far_rsem}[receiver]
        dst = {"near": near_in, "far": far_in}[receiver]
        return copy(far_out.at[s, rows(h)], dst.at[s, rows(h)], far_ssem.at[s, h], sem.at[s, h], far)

    def near_copy(h):
        s = spot(0)
        return copy(near_out.at[rows(h)], far_in.at[s, rows(h)], near_ssem.at[h], far_rsem.at[s, h], near)

    def near_arrival(t, h):
        s = spot(t)
        copy(far_out.at[s, rows(h)], near_in.at[s, rows(h)], far_ssem.at[s, h], near_rsem.at[s, h], far).wait_recv()

    def far_arrival(t, h):
        s = spot(t)
        copy(far_out.at[s, rows(h)], far_in.at[s, rows(h)], far_ssem.at[s, h], far_rsem.at[s, h], far).wait_recv()

    def sum_arrival(t):
        s = spot(t)
        copy(q_send.at[s], q_recv.at[s], q_ssem.at[s], q_rsem.at[s], partner).wait_recv()

    def own_part(s, r):
        return q_sum[k, s, r] + q_recv[s, r].astype(F32)

    def far_start(t):
        sum_arrival(t)
        s = spot(t)
        for h in range(CHUNKS):
            r = rows(h)
            far_out[s, r] = own_part(s, r).astype(BF16)
            far_copy(t, h, "near").start()

    def far_pass(t):
        sum_arrival(t)
        s = spot(t)
        for h in range(CHUNKS):
            r = rows(h)
            near_arrival(t, h)
            far_out[s, r] = (own_part(s, r) + near_in[s, r].astype(F32)).astype(BF16)
            far_copy(t, h, "far").start()

    def near_pass():
        sum_arrival(0)
        s = spot(0)
        for h in range(CHUNKS):
            r = rows(h)
            far_arrival(0, h)
            near_out[r] = (own_part(s, r) + far_in[s, r].astype(F32)).astype(BF16)
            near_copy(h).start()

    def back_begin(d):
        for h in range(SLICES):
            r = thin(h)
            p_send[d - 1, r] = p_sum[d, r].astype(BF16)
            back_start(d - 1, h)

    def back_pass(d):
        for h in range(SLICES):
            r = thin(h)
            back_copy(d, h).wait_recv()
            p_send[d - 1, r] = (p_sum[d, r] + p_recv[d, r].astype(F32)).astype(BF16)
            back_start(d - 1, h)

    def image_first(h):
        @pl.when(edge)
        def _():
            image_copy(0, h, img_fsem, far).start()
            image_copy(0, h, img_psem, partner).start()

        @pl.when(middle)
        def _():
            image_copy(1, h, img_fsem, far).start()
            image_copy(1, h, img_nsem, near).start()
            image_copy(1, h, img_psem, partner).start()

    def image_stage(u):
        for h in range(CHUNKS):
            @pl.when(edge)
            def _():
                image_arrival(k, spot(u + 1), h)
                image_copy(u + 1, h, img_psem, partner).start()

            @pl.when(middle)
            def _():
                if u == 0:
                    image_arrival(k, spot(0), h)
                    image_copy(0, h, img_fsem, far).start()
                    image_copy(0, h, img_psem, partner).start()
                else:
                    image_arrival(k, spot(u + 1), h)
                    image_copy(u + 1, h, img_nsem, near).start()
                    image_copy(u + 1, h, img_psem, partner).start()

    def text_stage(u):
        for h in range(SLICES):
            text_copy(u, h).wait_recv()
            if u == 0:
                text_start(1, h)
            elif u == 1:
                @pl.when(j >= 5)
                def _():
                    text_start(2, h)

    def weights(logits, gap):
        logits = LOGIT_SCALE * logits + BIAS_LOGIT
        row = lax.broadcasted_iota(jnp.int32, logits.shape, 0)
        col = lax.broadcasted_iota(jnp.int32, logits.shape, 1)
        gap = gap + 8 * (col // ROWS) + 4 * (row // ROWS)
        match = (gap == 0) & (lax.rem(row, ROWS) == lax.rem(col, ROWS))
        weight = jax.nn.sigmoid(jnp.where(match, -logits, logits))
        weight = jnp.where(match, -weight, weight)
        return jnp.where((gap >= 0) & (gap <= 19), weight, 0.0).astype(BF16)

    NT = (((1,), (1,)), ((), ()))
    TN = (((0,), (0,)), ((), ()))

    def products(t, first_text, texts):
        s = spot(t)
        part_w = wgt.at[:, pl.ds(0, texts * ROWS)]
        near_texts = pl.ds(first_text, texts)
        pair = img[:, s].reshape(2 * ROWS, WIDTH)
        block = txt[near_texts].reshape(texts * ROWS, WIDTH)
        logits = lax.dot_general(pair, block, NT, preferred_element_type=F32)
        part_w[...] = weights(logits, 8 * first_text + s - j)
        for n in range(WIDTH // COLS):
            part = pl.ds(n * COLS, COLS)
            block = txt[near_texts, :, part].reshape(texts * ROWS, COLS)
            q = jnp.dot(part_w[...], block, preferred_element_type=F32).reshape(2, ROWS, COLS)
            pair = img[:, s, :, part].reshape(2 * ROWS, COLS)
            p = lax.dot_general(part_w[...], pair, TN, preferred_element_type=F32)
            if first_text == 0:
                q_sum[:, s, :, part] = q
            else:
                q_sum[:, s, :, part] += q
            p_sum[near_texts, :, part] += p.reshape(texts, ROWS, COLS)

    def recent(t):
        s = spot(t)
        for h in range(CHUNKS):
            image_arrival(1 - k, s, h)
        products(t, 0, 2)

    def share(s):
        q_send[s] = q_sum[1 - k, s].astype(BF16)
        copy(q_send.at[s], q_recv.at[s], q_ssem.at[s], q_rsem.at[s], partner).start()

    def older(t):
        products(t, 2, 1)

        @pl.when((j < 5) | (spot(t) >= z))
        def _():
            share(spot(t))

    def oldest(start, stop):
        @pl.loop(start, stop)
        def _(s):
            old = weights(lax.dot_general(img[0, s], txt[3], NT, preferred_element_type=F32), 24 + s - j)
            q_sum[0, s] += jnp.dot(old, txt[3], preferred_element_type=F32)
            p_sum[3] += lax.dot_general(old, img[0, s], TN, preferred_element_type=F32)
            share(s)

    late = j >= 5
    soon = j < 5

    for h in range(CHUNKS // 2):
        image_first(h)
    when(relay & not_final & not_early, pl.semaphore_wait, fwd_ready, 1)
    when(relay & not_early, text_relay_stage, 0)
    when(relay & not_early, text_relay_stage, 1)
    for h in range(CHUNKS // 2, CHUNKS):
        image_first(h)
    p_sum[...] = jnp.zeros_like(p_sum)
    image_stage(0)
    when(relay & early, pl.semaphore_wait, fwd_ready, 1)
    when(relay & early, text_relay_stage, 0)
    when(relay & early, text_relay_stage, 1)
    when(middle, image_stage, 1)
    when(middle & first, image_stage, 2)
    text_stage(0)

    when(relay & late, text_relay_stage, 2)

    @pl.loop(0, 2 + z * (3 - z) // 2)
    def _(i):
        recent(jnp.where(i < 2, 1 - i, 2))

    when(edge, image_stage, 1)
    when(middle & jnp.logical_not(first), image_stage, 2)
    text_stage(1)
    when(edge, recent, 2)

    @pl.loop(0, 3)
    def _(i):
        older(2 - i)

    when(edge, image_stage, 2)

    @pl.when(late & edge)
    def _():
        text_stage(2)
        oldest(1, 3)

    when(edge, far_start, 2)
    recent(3)
    older(3)

    @pl.when(late & middle)
    def _():
        text_stage(2)

    @pl.when(late)
    def _():
        oldest(0, jnp.where(middle, z, 1))


    when(first, pl.semaphore_wait, lane_ready, SLICES)
    slow = last | (late & (place == 30))
    def relay_step(n, here):
        when(relay & late & here, back_relay_stage, 2 - n)
        if n < 2:
            when(relay & soon & here, back_relay_stage, 1 - n)

    when(late, back_begin, 3)
    when(soon, back_begin, 2)
    relay_step(0, not_early)
    when(edge, far_start, 3)
    when(late & jnp.logical_not(last), back_pass, 2)
    when(middle, far_pass, 2)
    when(relay & early, pl.semaphore_wait, back_ready, 1)
    relay_step(0, early)
    hold = relay & (z == 3)
    when(edge & jnp.logical_not(hold), far_start, 1)
    when(jnp.logical_not(slow), back_pass, 1)
    relay_step(1, not_early)
    when(middle, far_pass, 3)
    relay_step(1, early)
    when(hold, far_start, 1)
    relay_step(2, True)
    when(middle, near_pass)
    when(late & last, back_pass, 2)
    when(slow, back_pass, 1)
    when(edge, sum_arrival, 0)
    when(middle, sum_arrival, 1)

    for h in range(SLICES):
        back_copy(0, h).wait_recv()
    text_out[...] = undo(p_sum[0] + p_recv[0].astype(F32), text_ref)

    @pl.when(edge)
    def _():
        for h in range(CHUNKS):
            far_arrival(0, h)
        total = q_sum[k, z] + q_recv[z].astype(F32) + far_in[z].astype(F32)
        image_out[...] = undo(total, image_ref)

    @pl.when(middle)
    def _():
        for h in range(CHUNKS):
            near_arrival(1, h)
            far_arrival(1, h)
        total = q_sum[k, z] + q_recv[z].astype(F32) + near_in[z].astype(F32) + far_in[z].astype(F32)
        image_out[...] = undo(total, image_ref)

    for d in range(3):
        @pl.when(relay & (j >= 5) if d == 2 else relay)
        def _():
            text_relay(d).wait_send()
            back_relay(d).wait_send()

        @pl.when(j >= (5 if d == 2 else 0))
        def _():
            for h in range(SLICES):
                back_copy(d, h).wait_send()

        @pl.when((j >= (5 if d == 2 else 0)) & ((d == 0) | jnp.logical_not(last)))
        def _():
            for h in range(SLICES):
                text_copy(d, h).wait_send()

        if d < 2:
            @pl.when(ante & (j >= 5) if d == 1 else ante)
            def _():
                for h in range(SLICES):
                    ante_copy(d, h).wait_send()

    for h in range(CHUNKS):
        for t in range(4):
            image_copy(t, h, img_psem, partner).wait_send()

        @pl.when(edge)
        def _():
            image_copy(0, h, img_fsem, far).wait_send()
            for t in (1, 2, 3):
                far_copy(t, h, "near").wait_send()

        @pl.when(middle)
        def _():
            for t in (0, 1):
                image_copy(t, h, img_fsem, far).wait_send()
            for t in (1, 2, 3):
                image_copy(t, h, img_nsem, near).wait_send()
            for t in (2, 3):
                far_copy(t, h, "far").wait_send()
            near_copy(h).wait_send()

    @pl.loop(0, 4)
    def _(s):
        copy(q_send.at[s], q_recv.at[s], q_ssem.at[s], q_rsem.at[s], partner).wait_send()


def solution(mesh):
    blocks = mesh.shape["blk"]
    dma = pltpu.SemaphoreType.DMA
    block = (ROWS, WIDTH)

    def per_device(image_embeds, text_embeds):
        out = jax.ShapeDtypeStruct(block, BF16)
        vmem = pl.BlockSpec(memory_space=pltpu.VMEM)
        return pl.pallas_call(
            lambda *refs: kernel(blocks, *refs),
            out_shape=(out, out),
            in_specs=[pl.BlockSpec(memory_space=pl.ANY)] * 2,
            out_specs=(vmem, vmem),
            scratch_shapes=[
                pltpu.VMEM(block, BF16),
                pltpu.VMEM(block, BF16),
                dma((2,)),
                pltpu.VMEM((2, 4) + block, BF16),
                pltpu.VMEM((4,) + block, BF16),
                pltpu.VMEM((2 * ROWS, 3 * ROWS), BF16),
                pltpu.VMEM((2, 4) + block, F32),
                pltpu.VMEM((4,) + block, F32),
                pltpu.VMEM((4,) + block, BF16),
                pltpu.VMEM((4,) + block, BF16),
                pltpu.VMEM((4,) + block, BF16),
                pltpu.VMEM(block, BF16),
                pltpu.VMEM((4,) + block, BF16),
                pltpu.VMEM((4,) + block, BF16),
                pltpu.VMEM((3,) + block, BF16),
                pltpu.VMEM((3,) + block, BF16),
                pltpu.VMEM((3, THIN, WIDTH), BF16),
                pltpu.VMEM((3, THIN, WIDTH), BF16),
                dma((3, SLICES)),
                dma((3, SLICES)),
                dma((4, CHUNKS)),
                dma((4, CHUNKS)),
                dma((4, CHUNKS)),
                dma((2, 4, CHUNKS)),
                dma((4,)),
                dma((4,)),
                dma((4, CHUNKS)),
                dma((CHUNKS,)),
                dma((4, CHUNKS)),
                dma((4, CHUNKS)),
                dma((3, SLICES)),
                dma((3, SLICES)),
                dma((2, SLICES)),
                dma((3,)),
                dma((3,)),
                dma((3,)),
                dma((3,)),
                pltpu.SemaphoreType.REGULAR,
                pltpu.SemaphoreType.REGULAR,
                pltpu.SemaphoreType.REGULAR,
            ],
            compiler_params=pltpu.CompilerParams(
                collective_id=0, has_side_effects=True, vmem_limit_bytes=56 * 1024 * 1024
            ),
            name="pair_window",
        )(image_embeds, text_embeds)

    spec = P(("blk", "grp"), None)
    return jax.shard_map(
        per_device, mesh=mesh, in_specs=(spec, spec), out_specs=(spec, spec), check_vma=False
    )
```

```python
import jax
import jax.numpy as jnp
from jax import lax
from jax.experimental import pallas as pl
from jax.experimental.pallas import tpu as pltpu
from jax.sharding import PartitionSpec as P

MESH = pl.DeviceIdType.MESH
LOGIT_SCALE = 10.0
BIAS_LOGIT = -2.0
EPSILON = 1e-06
ROWS = 128
WIDTH = 1152
CHUNKS = 4
PIECE = ROWS // CHUNKS
SLICES = 8
THIN = ROWS // SLICES
RELAYS = ((26, 14, 17, 29, 2, 16, 7, 24), (9, 5, 22, 8, 6, 25, 15, 23))
COLS = 384
F32 = jnp.float32
BF16 = jnp.bfloat16


def unit_and_inverse(ref):
    wide = ref[...].astype(F32)
    length = jnp.sqrt(jnp.sum(wide * wide, axis=-1, keepdims=True) + EPSILON)
    inverse = 1.0 / length
    return wide * inverse, inverse


def undo(total, wide):
    wide = wide.astype(F32)
    inverse = 1.0 / jnp.sqrt(jnp.sum(wide * wide, axis=-1, keepdims=True) + EPSILON)
    unit = wide * inverse
    grad = LOGIT_SCALE * total
    inner = jnp.sum(unit * grad, axis=-1, keepdims=True)
    return ((grad - unit * inner) * inverse).astype(BF16)


def kernel(
    blocks,
    image_in, text_in, image_out, text_out,
    image_ref, text_ref, in_sem, out_held, out_sem,
    img, txt, wgt, q_sum, p_sum,
    q_send, q_recv, far_out, near_out, near_in, far_in, p_send, p_recv,
    fwd_hold, back_hold,
    txt_ssem, txt_rsem, img_fsem, img_nsem, img_psem, img_rsem, pair_rsem,
    q_ssem, q_rsem, far_ssem, near_ssem, near_rsem, far_rsem, p_ssem, p_rsem,
    ante_ssem, fwd_ssem, fwd_rsem, back_ssem, back_rsem, fwd_ready, back_ready, lane_ready,
):
    blk = lax.axis_index("blk")
    z = lax.axis_index("grp")
    k = lax.rem(blk, 2)
    j = 4 * k + z
    high = z // 2
    sign = 1 - 2 * high
    middle = (z == 1) | (z == 2)
    edge = (z == 0) | (z == 3)

    def spot(t):
        return 3 * high + sign * t

    column = blk // 2
    third = column // 32
    place = lax.rem(column, 32)
    first = place == 0
    last = place == 31
    ante = place == 30

    def relay_place(h):
        return RELAYS[0][h] + k * (RELAYS[1][h] - RELAYS[0][h])

    def at(hop, where):
        return (2 * (32 * lax.rem(third + hop, blocks // 64) + where) + k, z)

    role, relay = 0, False
    for h in range(SLICES):
        match = place == relay_place(h)
        role = role + jnp.where(match, h, 0)
        relay = relay | match
    next_first, own_first = at(1, 0), at(0, 0)
    prev_last, own_last, own_ante = at(blocks // 64 - 1, 31), at(0, 31), at(0, 30)

    partner = (blk + 1 - 2 * k, z)
    ahead = (lax.rem(blk + 2, blocks), z)
    behind = (lax.rem(blk + blocks - 2, blocks), z)
    far = (blk, z + sign)
    near = (blk, z - sign)

    def when(condition, run, *args):
        @pl.when(condition)
        def _():
            run(*args)

    def copy(src, dst, ssem, rsem, device):
        return pltpu.make_async_remote_copy(
            src_ref=src, dst_ref=dst, send_sem=ssem, recv_sem=rsem, device_id=device, device_id_type=MESH
        )

    def rows(h):
        return pl.ds(h * PIECE, PIECE)

    def thin(h):
        return pl.ds(pl.multiple_of(h * THIN, THIN), THIN)

    image_load = pltpu.make_async_copy(image_in, image_ref, in_sem.at[0])
    text_load = pltpu.make_async_copy(text_in, text_ref, in_sem.at[1])
    image_load.start()
    text_load.start()

    barrier = pltpu.get_barrier_semaphore()

    def greet(condition, devices):
        @pl.when(condition)
        def _():
            for device in devices:
                pl.semaphore_signal(barrier, inc=1, device_id=device, device_id_type=MESH)

    thirds = blocks // 64
    early, final = third == 0, third == thirds - 1
    not_early, not_final = jnp.logical_not(early), jnp.logical_not(final)
    past_relays = [at(thirds - 1, relay_place(h)) for h in range(SLICES)]
    coming_relays = [at(1, relay_place(h)) for h in range(SLICES)]
    own_relays = [at(0, relay_place(h)) for h in range(SLICES)]
    greet(relay, (own_last, own_ante))
    greet(first, own_relays)
    greet(first & early, past_relays)
    greet(last & not_final, coming_relays)
    greet(relay & not_final, (next_first,))
    greet(relay & early, (prev_last,))
    for device in (partner, far):
        pl.semaphore_signal(barrier, inc=1, device_id=device, device_id_type=MESH)
    greet(middle, (near,))
    greet(jnp.logical_not(first), (behind,))
    greet(jnp.logical_not(last), (ahead,))

    image_load.wait()
    unit, _ = unit_and_inverse(image_ref)
    img[k, z] = unit.astype(BF16)
    text_load.wait()
    unit, _ = unit_and_inverse(text_ref)
    txt[0] = unit.astype(BF16)

    answer_first, answer_last = first & not_early, last & final
    greeted = 4 + z * (3 - z) // 2 + jnp.where(last, SLICES - 1, 0) - jnp.where(first, 1, 0)
    greeted = greeted + jnp.where(answer_first | answer_last | ante, SLICES, 0)
    greeted = greeted + jnp.where(relay & final, 1, 0) + jnp.where(relay & not_early, 1, 0) + jnp.where(relay, 1, 0)
    pl.semaphore_wait(barrier, greeted)

    when(relay, lambda: pl.semaphore_signal(lane_ready, inc=1, device_id=own_first, device_id_type=MESH))

    @pl.when(answer_first)
    def _():
        for device in past_relays:
            pl.semaphore_signal(fwd_ready, inc=1, device_id=device, device_id_type=MESH)

    @pl.when(answer_last)
    def _():
        for device in coming_relays:
            pl.semaphore_signal(back_ready, inc=1, device_id=device, device_id_type=MESH)

    def image_copy(t, h, ssem, device):
        s = spot(t)
        ref = img.at[k, s, rows(h)]
        return copy(ref, ref, ssem.at[t], img_rsem.at[s, h], device)

    def to_partner(t, h):
        s = spot(t)
        ref = img.at[k, s, rows(h)]
        copy(ref, ref, img_psem.at[t], pair_rsem.at[s], partner).start()

    def image_arrival(s, h):
        ref = img.at[k, s, rows(h)]
        copy(ref, ref, img_psem.at[0], img_rsem.at[s, h], partner).wait_recv()

    def text_copy(d, h):
        return copy(
            txt.at[d, thin(h)], txt.at[d + 1, thin(h)], txt_ssem.at[d], txt_rsem.at[d, h], ahead
        )

    def relay_copy(d, hold, h, ssem):
        return copy(txt.at[d, thin(h)], fwd_hold.at[hold], ssem, fwd_rsem.at[hold], at(0, relay_place(h)))

    def ante_copy(d, h):
        return relay_copy(d, d + 1, h, ante_ssem.at[d])

    def text_start(d, h):
        @pl.when(jnp.logical_not(last))
        def _():
            text_copy(d, h).start()

        if d == 0:
            @pl.when(last)
            def _():
                relay_copy(0, 0, h, txt_ssem.at[0]).start()

    def text_relay(d):
        return copy(
            fwd_hold.at[d], txt.at[d + 1, thin(role)], fwd_ssem.at[d], txt_rsem.at[d, role], next_first
        )

    def text_relay_stage(d):
        copy(fwd_hold.at[d], fwd_hold.at[d], fwd_ssem.at[d], fwd_rsem.at[d], next_first).wait_recv()
        text_relay(d).start()

    for h in range(SLICES):
        when(ante, lambda h=h: ante_copy(0, h).start())

    for h in range(SLICES):
        text_start(0, h)

    def back_copy(d, h):
        return copy(p_send.at[d, thin(h)], p_recv.at[d, thin(h)], p_ssem.at[d], p_rsem.at[d, h], behind)

    def back_start(d, h):
        @pl.when(first)
        def _():
            copy(
                p_send.at[d, thin(h)], back_hold.at[d], p_ssem.at[d], back_rsem.at[d], at(0, relay_place(h))
            ).start()

        @pl.when(jnp.logical_not(first))
        def _():
            back_copy(d, h).start()

    def back_relay(d):
        return copy(
            back_hold.at[d], p_recv.at[d, thin(role)], back_ssem.at[d], p_rsem.at[d, role], prev_last
        )

    def back_relay_stage(d):
        copy(back_hold.at[d], back_hold.at[d], back_ssem.at[d], back_rsem.at[d], prev_last).wait_recv()
        back_relay(d).start()

    def far_copy(t, h, receiver):
        s = spot(t)
        sem = {"near": near_rsem, "far": far_rsem}[receiver]
        dst = {"near": near_in, "far": far_in}[receiver]
        return copy(far_out.at[s, rows(h)], dst.at[s, rows(h)], far_ssem.at[s], sem.at[s, h], far)

    def near_copy(h):
        s = spot(0)
        return copy(near_out.at[rows(h)], far_in.at[s, rows(h)], near_ssem, far_rsem.at[s, h], near)

    def near_arrival(t, h):
        s = spot(t)
        copy(far_out.at[s, rows(h)], near_in.at[s, rows(h)], far_ssem.at[s], near_rsem.at[s, h], far).wait_recv()

    def far_arrival(t, h):
        s = spot(t)
        copy(far_out.at[s, rows(h)], far_in.at[s, rows(h)], far_ssem.at[s], far_rsem.at[s, h], far).wait_recv()

    def sum_arrival(t):
        s = spot(t)
        copy(q_send.at[s], q_recv.at[s], q_ssem.at[s], q_rsem.at[s], partner).wait_recv()

    def own_part(s, r):
        return q_sum[k, s, r] + q_recv[s, r].astype(F32)

    def far_start(t):
        sum_arrival(t)
        s = spot(t)
        for h in range(CHUNKS):
            r = rows(h)
            far_out[s, r] = own_part(s, r).astype(BF16)
            far_copy(t, h, "near").start()

    def far_pass(t):
        sum_arrival(t)
        s = spot(t)
        for h in range(CHUNKS):
            r = rows(h)
            near_arrival(t, h)
            far_out[s, r] = (own_part(s, r) + near_in[s, r].astype(F32)).astype(BF16)
            far_copy(t, h, "far").start()

    def near_pass():
        sum_arrival(0)
        s = spot(0)
        for h in range(CHUNKS):
            r = rows(h)
            far_arrival(0, h)
            near_out[r] = (own_part(s, r) + far_in[s, r].astype(F32)).astype(BF16)
            near_copy(h).start()

    def back_begin(d):
        for h in range(SLICES):
            r = thin(h)
            p_send[d - 1, r] = p_sum[d, r].astype(BF16)
            back_start(d - 1, h)

    def back_pass(d):
        for h in range(SLICES):
            r = thin(h)
            back_copy(d, h).wait_recv()
            p_send[d - 1, r] = (p_sum[d, r] + p_recv[d, r].astype(F32)).astype(BF16)
            back_start(d - 1, h)

    def image_first(h):
        @pl.when(edge)
        def _():
            image_copy(0, h, img_fsem, far).start()
            to_partner(0, h)

        @pl.when(middle)
        def _():
            image_copy(1, h, img_fsem, far).start()
            image_copy(1, h, img_nsem, near).start()
            to_partner(1, h)

    def image_stage(u):
        for h in range(CHUNKS):
            @pl.when(edge)
            def _():
                image_arrival(spot(u + 1), h)
                to_partner(u + 1, h)

            @pl.when(middle)
            def _():
                if u == 0:
                    image_arrival(spot(0), h)
                    image_copy(0, h, img_fsem, far).start()
                    to_partner(0, h)
                else:
                    image_arrival(spot(u + 1), h)
                    image_copy(u + 1, h, img_nsem, near).start()
                    to_partner(u + 1, h)

    def text_stage(u):
        for h in range(SLICES):
            text_copy(u, h).wait_recv()
            if u == 0:
                when(ante & (j >= 5), lambda h=h: ante_copy(1, h).start())
                when(jnp.logical_not(ante & (j >= 5)), text_start, 1, h)
            elif u == 1:
                @pl.when(j >= 5)
                def _():
                    text_start(2, h)

        if u == 0:
            @pl.when(ante & (j >= 5))
            def _():
                for h in range(SLICES):
                    text_start(1, h)

    def weights(logits, gap):
        logits = LOGIT_SCALE * logits + BIAS_LOGIT
        row = lax.broadcasted_iota(jnp.int32, logits.shape, 0)
        col = lax.broadcasted_iota(jnp.int32, logits.shape, 1)
        gap = gap + 8 * (col // ROWS) + 4 * (row // ROWS)
        match = (gap == 0) & (lax.rem(row, ROWS) == lax.rem(col, ROWS))
        weight = jax.nn.sigmoid(jnp.where(match, -logits, logits))
        weight = jnp.where(match, -weight, weight)
        return jnp.where((gap >= 0) & (gap <= 19), weight, 0.0).astype(BF16)

    NT = (((1,), (1,)), ((), ()))
    TN = (((0,), (0,)), ((), ()))

    def products(t, first_text, texts):
        s = spot(t)
        part_w = wgt.at[:, pl.ds(0, texts * ROWS)]
        near_texts = pl.ds(first_text, texts)
        pair = img[:, s].reshape(2 * ROWS, WIDTH)
        block = txt[near_texts].reshape(texts * ROWS, WIDTH)
        logits = lax.dot_general(pair, block, NT, preferred_element_type=F32)
        part_w[...] = weights(logits, 8 * first_text + s - j)
        for n in range(WIDTH // COLS):
            part = pl.ds(n * COLS, COLS)
            block = txt[near_texts, :, part].reshape(texts * ROWS, COLS)
            q = jnp.dot(part_w[...], block, preferred_element_type=F32).reshape(2, ROWS, COLS)
            pair = img[:, s, :, part].reshape(2 * ROWS, COLS)
            p = lax.dot_general(part_w[...], pair, TN, preferred_element_type=F32)
            if first_text == 0:
                q_sum[:, s, :, part] = q
            else:
                q_sum[:, s, :, part] += q
            p_sum[near_texts, :, part] += p.reshape(texts, ROWS, COLS)

    def recent(t):
        s = spot(t)
        ref = img.at[1 - k, s]
        copy(ref, ref, img_psem.at[t], pair_rsem.at[s], partner).wait_recv()
        products(t, 0, 2)

    def share(s):
        q_send[s] = q_sum[1 - k, s].astype(BF16)
        copy(q_send.at[s], q_recv.at[s], q_ssem.at[s], q_rsem.at[s], partner).start()

    def older(t):
        products(t, 2, 1)

        @pl.when((j < 5) | (spot(t) >= z))
        def _():
            share(spot(t))

    def oldest(start, stop):
        @pl.loop(start, stop)
        def _(s):
            old = weights(lax.dot_general(img[0, s], txt[3], NT, preferred_element_type=F32), 24 + s - j)
            q_sum[0, s] += jnp.dot(old, txt[3], preferred_element_type=F32)
            p_sum[3] += lax.dot_general(old, img[0, s], TN, preferred_element_type=F32)
            share(s)

    late = j >= 5
    soon = j < 5

    for h in range(CHUNKS // 2):
        image_first(h)
    when(relay & not_final & not_early, pl.semaphore_wait, fwd_ready, 1)
    when(relay & not_early, text_relay_stage, 0)
    when(relay & not_early, text_relay_stage, 1)
    for h in range(CHUNKS // 2, CHUNKS):
        image_first(h)
    p_sum[...] = jnp.zeros_like(p_sum)
    image_stage(0)
    when(relay & early, pl.semaphore_wait, fwd_ready, 1)
    when(relay & early, text_relay_stage, 0)
    when(relay & early, text_relay_stage, 1)
    when(middle, image_stage, 1)
    when(middle & first, image_stage, 2)
    text_stage(0)

    when(relay & late, text_relay_stage, 2)

    @pl.loop(0, 2 + z * (3 - z) // 2)
    def _(i):
        recent(jnp.where(i < 2, 1 - i, 2))

    when(edge, image_stage, 1)
    when(middle & jnp.logical_not(first), image_stage, 2)
    text_stage(1)
    when(edge, recent, 2)

    @pl.loop(0, 3)
    def _(i):
        older(2 - i)

    when(edge, image_stage, 2)

    @pl.when(late & edge)
    def _():
        text_stage(2)
        oldest(1, 3)

    when(edge, far_start, 2)
    recent(3)
    older(3)

    @pl.when(late & middle)
    def _():
        text_stage(2)

    @pl.when(late)
    def _():
        oldest(0, jnp.where(middle, z, 1))


    when(first, pl.semaphore_wait, lane_ready, SLICES)
    slow = last | (late & (place == 30))
    def relay_step(n, here):
        when(relay & late & here, back_relay_stage, 2 - n)
        if n < 2:
            when(relay & soon & here, back_relay_stage, 1 - n)

    when(late, back_begin, 3)
    when(soon, back_begin, 2)
    relay_step(0, not_early)
    when(edge, far_start, 3)
    when(late & jnp.logical_not(last), back_pass, 2)
    when(middle, far_pass, 2)
    when(relay & early, pl.semaphore_wait, back_ready, 1)
    relay_step(0, early)
    hold = relay & (z == 3)
    when(edge & jnp.logical_not(hold), far_start, 1)
    when(jnp.logical_not(slow), back_pass, 1)
    relay_step(1, not_early)
    when(middle, far_pass, 3)
    relay_step(1, early)
    when(hold, far_start, 1)
    relay_step(2, True)
    when(middle, near_pass)
    when(late & last, back_pass, 2)
    when(slow, back_pass, 1)
    when(edge, sum_arrival, 0)
    when(middle, sum_arrival, 1)

    def finish(which, h, total):
        r = rows(h)
        out_held[which, r] = undo(total, (image_ref, text_ref)[which][r])
        out_copy(which, h).start()

    def out_copy(which, h):
        r = rows(h)
        return pltpu.make_async_copy(out_held.at[which, r], (image_out, text_out)[which].at[r], out_sem.at[which])

    for h in range(CHUNKS):
        for i in range(SLICES // CHUNKS):
            back_copy(0, SLICES // CHUNKS * h + i).wait_recv()
        finish(1, h, p_sum[0, rows(h)] + p_recv[0, rows(h)].astype(F32))

    for h in range(CHUNKS):
        r = rows(h)

        @pl.when(edge)
        def _():
            far_arrival(0, h)
            finish(0, h, own_part(z, r) + far_in[z, r].astype(F32))

        @pl.when(middle)
        def _():
            near_arrival(1, h)
            far_arrival(1, h)
            finish(0, h, own_part(z, r) + near_in[z, r].astype(F32) + far_in[z, r].astype(F32))

    def sent(block, ssem):
        copy(block, block, ssem, img_rsem.at[0, 0], partner).wait_send()

    for which in range(2):
        pltpu.make_async_copy(out_held.at[which], (image_out, text_out)[which], out_sem.at[which]).wait()

    for d in range(3):
        used = late if d == 2 else True
        when(relay & used, lambda: text_relay(d).wait_send())
        when(relay & used, lambda: back_relay(d).wait_send())
        when((j >= 0) & used, sent, p_send.at[d], p_ssem.at[d])
        when((j >= 0) & used if d == 0 else jnp.logical_not(last) & used, sent, txt.at[d], txt_ssem.at[d])
        if d < 2:
            when(ante & (late if d == 1 else True), sent, txt.at[d], ante_ssem.at[d])

    for t in range(4):
        sent(img.at[k, spot(t)], img_psem.at[t])

    @pl.when(edge)
    def _():
        sent(img.at[k, spot(0)], img_fsem.at[0])
        for t in (1, 2, 3):
            sent(far_out.at[spot(t)], far_ssem.at[spot(t)])

    @pl.when(middle)
    def _():
        for t in (0, 1):
            sent(img.at[k, spot(t)], img_fsem.at[t])
        for t in (1, 2, 3):
            sent(img.at[k, spot(t)], img_nsem.at[t])
        for t in (2, 3):
            sent(far_out.at[spot(t)], far_ssem.at[spot(t)])
        sent(near_out, near_ssem)

    @pl.loop(0, 4)
    def _(s):
        sent(q_send.at[s], q_ssem.at[s])


def solution(mesh):
    blocks = mesh.shape["blk"]
    dma = pltpu.SemaphoreType.DMA
    block = (ROWS, WIDTH)

    def per_device(image_embeds, text_embeds):
        out = jax.ShapeDtypeStruct(block, BF16)
        anywhere = pl.BlockSpec(memory_space=pl.ANY)
        return pl.pallas_call(
            lambda *refs: kernel(blocks, *refs),
            out_shape=(out, out),
            in_specs=[anywhere] * 2,
            out_specs=(anywhere, anywhere),
            scratch_shapes=[
                pltpu.VMEM(block, BF16),
                pltpu.VMEM(block, BF16),
                dma((2,)),
                pltpu.VMEM((2,) + block, BF16),
                dma((2,)),
                pltpu.VMEM((2, 4) + block, BF16),
                pltpu.VMEM((4,) + block, BF16),
                pltpu.VMEM((2 * ROWS, 3 * ROWS), BF16),
                pltpu.VMEM((2, 4) + block, F32),
                pltpu.VMEM((4,) + block, F32),
                pltpu.VMEM((4,) + block, BF16),
                pltpu.VMEM((4,) + block, BF16),
                pltpu.VMEM((4,) + block, BF16),
                pltpu.VMEM(block, BF16),
                pltpu.VMEM((4,) + block, BF16),
                pltpu.VMEM((4,) + block, BF16),
                pltpu.VMEM((3,) + block, BF16),
                pltpu.VMEM((3,) + block, BF16),
                pltpu.VMEM((3, THIN, WIDTH), BF16),
                pltpu.VMEM((3, THIN, WIDTH), BF16),
                dma((3,)),
                dma((3, SLICES)),
                dma((4,)),
                dma((4,)),
                dma((4,)),
                dma((4, CHUNKS)),
                dma((4,)),
                dma((4,)),
                dma((4,)),
                dma((4,)),
                dma(()),
                dma((4, CHUNKS)),
                dma((4, CHUNKS)),
                dma((3,)),
                dma((3, SLICES)),
                dma((2,)),
                dma((3,)),
                dma((3,)),
                dma((3,)),
                dma((3,)),
                pltpu.SemaphoreType.REGULAR,
                pltpu.SemaphoreType.REGULAR,
                pltpu.SemaphoreType.REGULAR,
            ],
            compiler_params=pltpu.CompilerParams(
                collective_id=0, has_side_effects=True, vmem_limit_bytes=56 * 1024 * 1024
            ),
            name="pair_window",
        )(image_embeds, text_embeds)

    spec = P(("blk", "grp"), None)
    return jax.shard_map(
        per_device, mesh=mesh, in_specs=(spec, spec), out_specs=(spec, spec), check_vma=False
    )
```

```python
import jax
import jax.numpy as jnp
from jax import lax
from jax.experimental import pallas as pl
from jax.experimental.pallas import tpu as pltpu
from jax.sharding import PartitionSpec as P

MESH = pl.DeviceIdType.MESH
LOGIT_SCALE = 10.0
BIAS_LOGIT = -2.0
EPSILON = 1e-06
ROWS = 128
WIDTH = 1152
CHUNKS = 4
PIECE = ROWS // CHUNKS
SLICES = 8
THIN = ROWS // SLICES
RELAYS = ((26, 14, 17, 29, 2, 16, 7, 24), (9, 5, 22, 8, 6, 25, 15, 23))
COLS = 384
F32 = jnp.float32
BF16 = jnp.bfloat16


def unit_and_inverse(ref):
    wide = ref[...].astype(F32)
    length = jnp.sqrt(jnp.sum(wide * wide, axis=-1, keepdims=True) + EPSILON)
    inverse = 1.0 / length
    return wide * inverse, inverse


def undo(total, wide):
    wide = wide.astype(F32)
    inverse = 1.0 / jnp.sqrt(jnp.sum(wide * wide, axis=-1, keepdims=True) + EPSILON)
    unit = wide * inverse
    grad = LOGIT_SCALE * total
    inner = jnp.sum(unit * grad, axis=-1, keepdims=True)
    return ((grad - unit * inner) * inverse).astype(BF16)


def kernel(
    blocks,
    image_in, text_in, image_out, text_out,
    image_ref, text_ref, in_sem, out_held, out_sem,
    img, txt, wgt, q_sum, p_sum,
    q_send, q_recv, far_out, near_out, near_in, far_in, p_send, p_recv,
    fwd_hold, back_hold,
    txt_ssem, txt_rsem, img_fsem, img_nsem, img_psem, img_rsem, pair_rsem,
    q_ssem, q_rsem, far_ssem, near_ssem, near_rsem, far_rsem, p_ssem, p_rsem,
    ante_ssem, fwd_ssem, fwd_rsem, back_ssem, back_rsem, fwd_ready, back_ready, lane_ready,
):
    blk = lax.axis_index("blk")
    z = lax.axis_index("grp")
    k = lax.rem(blk, 2)
    j = 4 * k + z
    high = z // 2
    sign = 1 - 2 * high
    middle = (z == 1) | (z == 2)
    edge = (z == 0) | (z == 3)

    def spot(t):
        return 3 * high + sign * t

    column = blk // 2
    third = column // 32
    place = lax.rem(column, 32)
    first = place == 0
    last = place == 31
    ante = place == 30

    def relay_place(h):
        return RELAYS[0][h] + k * (RELAYS[1][h] - RELAYS[0][h])

    def at(hop, where):
        return (2 * (32 * lax.rem(third + hop, blocks // 64) + where) + k, z)

    role, relay = 0, False
    for h in range(SLICES):
        match = place == relay_place(h)
        role = role + jnp.where(match, h, 0)
        relay = relay | match
    next_first, own_first = at(1, 0), at(0, 0)
    prev_last, own_last, own_ante = at(blocks // 64 - 1, 31), at(0, 31), at(0, 30)

    partner = (blk + 1 - 2 * k, z)
    ahead = (lax.rem(blk + 2, blocks), z)
    behind = (lax.rem(blk + blocks - 2, blocks), z)
    far = (blk, z + sign)
    near = (blk, z - sign)

    def when(condition, run, *args):
        @pl.when(condition)
        def _():
            run(*args)

    def copy(src, dst, ssem, rsem, device):
        return pltpu.make_async_remote_copy(
            src_ref=src, dst_ref=dst, send_sem=ssem, recv_sem=rsem, device_id=device, device_id_type=MESH
        )

    def rows(h):
        return pl.ds(h * PIECE, PIECE)

    def thin(h):
        return pl.ds(pl.multiple_of(h * THIN, THIN), THIN)

    image_load = pltpu.make_async_copy(image_in, image_ref, in_sem.at[0])
    text_load = pltpu.make_async_copy(text_in, text_ref, in_sem.at[1])
    image_load.start()
    text_load.start()

    barrier = pltpu.get_barrier_semaphore()

    def greet(condition, devices):
        @pl.when(condition)
        def _():
            for device in devices:
                pl.semaphore_signal(barrier, inc=1, device_id=device, device_id_type=MESH)

    thirds = blocks // 64
    early, final = third == 0, third == thirds - 1
    not_early, not_final = jnp.logical_not(early), jnp.logical_not(final)
    past_relays = [at(thirds - 1, relay_place(h)) for h in range(SLICES)]
    coming_relays = [at(1, relay_place(h)) for h in range(SLICES)]
    own_relays = [at(0, relay_place(h)) for h in range(SLICES)]
    greet(relay, (own_last, own_ante))
    greet(first, own_relays)
    greet(first & early, past_relays)
    greet(last & not_final, coming_relays)
    greet(relay & not_final, (next_first,))
    greet(relay & early, (prev_last,))
    for device in (partner, far):
        pl.semaphore_signal(barrier, inc=1, device_id=device, device_id_type=MESH)
    greet(middle, (near,))
    greet(jnp.logical_not(first), (behind,))
    greet(jnp.logical_not(last), (ahead,))

    image_load.wait()
    unit, _ = unit_and_inverse(image_ref)
    img[k, z] = unit.astype(BF16)
    text_load.wait()
    unit, _ = unit_and_inverse(text_ref)
    txt[0] = unit.astype(BF16)

    answer_first, answer_last = first & not_early, last & final
    greeted = 4 + z * (3 - z) // 2 + jnp.where(last, SLICES - 1, 0) - jnp.where(first, 1, 0)
    greeted = greeted + jnp.where(answer_first | answer_last | ante, SLICES, 0)
    greeted = greeted + jnp.where(relay & final, 1, 0) + jnp.where(relay & not_early, 1, 0) + jnp.where(relay, 1, 0)
    pl.semaphore_wait(barrier, greeted)

    when(relay, lambda: pl.semaphore_signal(lane_ready, inc=1, device_id=own_first, device_id_type=MESH))

    @pl.when(answer_first)
    def _():
        for device in past_relays:
            pl.semaphore_signal(fwd_ready, inc=1, device_id=device, device_id_type=MESH)

    @pl.when(answer_last)
    def _():
        for device in coming_relays:
            pl.semaphore_signal(back_ready, inc=1, device_id=device, device_id_type=MESH)

    def image_copy(t, h, ssem, device):
        s = spot(t)
        ref = img.at[k, s, rows(h)]
        return copy(ref, ref, ssem.at[t], img_rsem.at[s, h], device)

    def to_partner(t, h):
        s = spot(t)
        ref = img.at[k, s, rows(h)]
        copy(ref, ref, img_psem.at[t], pair_rsem.at[s], partner).start()

    def image_arrival(s, h):
        ref = img.at[k, s, rows(h)]
        copy(ref, ref, img_psem.at[0], img_rsem.at[s, h], partner).wait_recv()

    def text_copy(d, h):
        return copy(
            txt.at[d, thin(h)], txt.at[d + 1, thin(h)], txt_ssem.at[d], txt_rsem.at[d, h // 2], ahead
        )

    def text_arrival(d, g):
        ref = txt.at[d + 1, rows(g)]
        copy(ref, ref, txt_ssem.at[d], txt_rsem.at[d, g], ahead).wait_recv()

    def back_arrival(d, g):
        ref = p_recv.at[d, rows(g)]
        copy(ref, ref, p_ssem.at[d], p_rsem.at[d, g], behind).wait_recv()

    def relay_copy(d, hold, h, ssem):
        return copy(txt.at[d, thin(h)], fwd_hold.at[hold], ssem, fwd_rsem.at[hold], at(0, relay_place(h)))

    def ante_copy(d, h):
        return relay_copy(d, d + 1, h, ante_ssem.at[d])

    def text_start(d, h):
        @pl.when(jnp.logical_not(last))
        def _():
            text_copy(d, h).start()

        if d == 0:
            @pl.when(last)
            def _():
                relay_copy(0, 0, h, txt_ssem.at[0]).start()

    def text_relay(d):
        return copy(
            fwd_hold.at[d], txt.at[d + 1, thin(role)], fwd_ssem.at[d], txt_rsem.at[d, role // 2], next_first
        )

    def text_relay_stage(d):
        copy(fwd_hold.at[d], fwd_hold.at[d], fwd_ssem.at[d], fwd_rsem.at[d], next_first).wait_recv()
        text_relay(d).start()

    for h in range(SLICES):
        when(ante, lambda h=h: ante_copy(0, h).start())

    for h in range(SLICES):
        text_start(0, h)

    def back_copy(d, h):
        return copy(p_send.at[d, thin(h)], p_recv.at[d, thin(h)], p_ssem.at[d], p_rsem.at[d, h // 2], behind)

    def back_start(d, h):
        @pl.when(first)
        def _():
            copy(
                p_send.at[d, thin(h)], back_hold.at[d], p_ssem.at[d], back_rsem.at[d], at(0, relay_place(h))
            ).start()

        @pl.when(jnp.logical_not(first))
        def _():
            back_copy(d, h).start()

    def back_relay(d):
        return copy(
            back_hold.at[d], p_recv.at[d, thin(role)], back_ssem.at[d], p_rsem.at[d, role // 2], prev_last
        )

    def back_relay_stage(d):
        copy(back_hold.at[d], back_hold.at[d], back_ssem.at[d], back_rsem.at[d], prev_last).wait_recv()
        back_relay(d).start()

    def far_copy(t, h, receiver):
        s = spot(t)
        sem = {"near": near_rsem, "far": far_rsem}[receiver]
        dst = {"near": near_in, "far": far_in}[receiver]
        return copy(far_out.at[s, rows(h)], dst.at[s, rows(h)], far_ssem.at[s], sem.at[s, h], far)

    def near_copy(h):
        s = spot(0)
        return copy(near_out.at[rows(h)], far_in.at[s, rows(h)], near_ssem, far_rsem.at[s, h], near)

    def near_arrival(t, h):
        s = spot(t)
        copy(far_out.at[s, rows(h)], near_in.at[s, rows(h)], far_ssem.at[s], near_rsem.at[s, h], far).wait_recv()

    def far_arrival(t, h):
        s = spot(t)
        copy(far_out.at[s, rows(h)], far_in.at[s, rows(h)], far_ssem.at[s], far_rsem.at[s, h], far).wait_recv()

    def sum_arrival(t):
        s = spot(t)
        copy(q_send.at[s], q_recv.at[s], q_ssem.at[s], q_rsem.at[s], partner).wait_recv()

    def own_part(s, r):
        return q_sum[k, s, r] + q_recv[s, r].astype(F32)

    def far_start(t):
        sum_arrival(t)
        s = spot(t)
        for h in range(CHUNKS):
            r = rows(h)
            far_out[s, r] = own_part(s, r).astype(BF16)
            far_copy(t, h, "near").start()

    def far_pass(t):
        sum_arrival(t)
        s = spot(t)
        for h in range(CHUNKS):
            r = rows(h)
            near_arrival(t, h)
            far_out[s, r] = (own_part(s, r) + near_in[s, r].astype(F32)).astype(BF16)
            far_copy(t, h, "far").start()

    def near_pass():
        sum_arrival(0)
        s = spot(0)
        for h in range(CHUNKS):
            r = rows(h)
            far_arrival(0, h)
            near_out[r] = (own_part(s, r) + far_in[s, r].astype(F32)).astype(BF16)
            near_copy(h).start()

    def back_begin(d):
        for h in range(SLICES):
            r = thin(h)
            p_send[d - 1, r] = p_sum[d, r].astype(BF16)
            back_start(d - 1, h)

    def back_pass(d):
        for g in range(CHUNKS):
            r = rows(g)
            back_arrival(d, g)
            p_send[d - 1, r] = (p_sum[d, r] + p_recv[d, r].astype(F32)).astype(BF16)
            back_start(d - 1, 2 * g)
            back_start(d - 1, 2 * g + 1)

    def image_first(h):
        @pl.when(edge)
        def _():
            image_copy(0, h, img_fsem, far).start()
            to_partner(0, h)

        @pl.when(middle)
        def _():
            image_copy(1, h, img_fsem, far).start()
            image_copy(1, h, img_nsem, near).start()
            to_partner(1, h)

    def image_stage(u):
        for h in range(CHUNKS):
            @pl.when(edge)
            def _():
                image_arrival(spot(u + 1), h)
                to_partner(u + 1, h)

            @pl.when(middle)
            def _():
                if u == 0:
                    image_arrival(spot(0), h)
                    image_copy(0, h, img_fsem, far).start()
                    to_partner(0, h)
                else:
                    image_arrival(spot(u + 1), h)
                    image_copy(u + 1, h, img_nsem, near).start()
                    to_partner(u + 1, h)

    def text_stage(u):
        for h in range(SLICES):
            if h % 2 == 0:
                text_arrival(u, h // 2)
            if u == 0:
                when(ante & (j >= 5), lambda h=h: ante_copy(1, h).start())
                when(jnp.logical_not(ante & (j >= 5)), text_start, 1, h)
            elif u == 1:
                @pl.when(j >= 5)
                def _():
                    text_start(2, h)

        if u == 0:
            @pl.when(ante & (j >= 5))
            def _():
                for h in range(SLICES):
                    text_start(1, h)

    def weights(logits, gap):
        logits = LOGIT_SCALE * logits + BIAS_LOGIT
        row = lax.broadcasted_iota(jnp.int32, logits.shape, 0)
        col = lax.broadcasted_iota(jnp.int32, logits.shape, 1)
        gap = gap + 8 * (col // ROWS) + 4 * (row // ROWS)
        match = (gap == 0) & (lax.rem(row, ROWS) == lax.rem(col, ROWS))
        weight = jax.nn.sigmoid(jnp.where(match, -logits, logits))
        weight = jnp.where(match, -weight, weight)
        return jnp.where((gap >= 0) & (gap <= 19), weight, 0.0).astype(BF16)

    NT = (((1,), (1,)), ((), ()))
    TN = (((0,), (0,)), ((), ()))

    def products(t, first_text, texts):
        s = spot(t)
        part_w = wgt.at[:, pl.ds(0, texts * ROWS)]
        near_texts = pl.ds(first_text, texts)
        pair = img[:, s].reshape(2 * ROWS, WIDTH)
        block = txt[near_texts].reshape(texts * ROWS, WIDTH)
        logits = lax.dot_general(pair, block, NT, preferred_element_type=F32)
        part_w[...] = weights(logits, 8 * first_text + s - j)
        for n in range(WIDTH // COLS):
            part = pl.ds(n * COLS, COLS)
            block = txt[near_texts, :, part].reshape(texts * ROWS, COLS)
            q = jnp.dot(part_w[...], block, preferred_element_type=F32).reshape(2, ROWS, COLS)
            pair = img[:, s, :, part].reshape(2 * ROWS, COLS)
            p = lax.dot_general(part_w[...], pair, TN, preferred_element_type=F32)
            if first_text == 0:
                q_sum[:, s, :, part] = q
            else:
                q_sum[:, s, :, part] += q
            p_sum[near_texts, :, part] += p.reshape(texts, ROWS, COLS)

    def recent(t):
        s = spot(t)
        ref = img.at[1 - k, s]
        copy(ref, ref, img_psem.at[t], pair_rsem.at[s], partner).wait_recv()
        products(t, 0, 2)

    def share(s):
        q_send[s] = q_sum[1 - k, s].astype(BF16)
        copy(q_send.at[s], q_recv.at[s], q_ssem.at[s], q_rsem.at[s], partner).start()

    def older(t):
        products(t, 2, 1)

        @pl.when((j < 5) | (spot(t) >= z))
        def _():
            share(spot(t))

    def oldest(start, stop):
        @pl.loop(start, stop)
        def _(s):
            old = weights(lax.dot_general(img[0, s], txt[3], NT, preferred_element_type=F32), 24 + s - j)
            q_sum[0, s] += jnp.dot(old, txt[3], preferred_element_type=F32)
            p_sum[3] += lax.dot_general(old, img[0, s], TN, preferred_element_type=F32)
            share(s)

    late = j >= 5
    soon = j < 5

    favoured = relay & final
    for h in range(CHUNKS // 2):
        when(jnp.logical_not(favoured), image_first, h)
    when(relay & not_final & not_early, pl.semaphore_wait, fwd_ready, 1)
    when(relay & not_early, text_relay_stage, 0)
    when(relay & not_early, text_relay_stage, 1)
    for h in range(CHUNKS // 2):
        when(favoured, image_first, h)
    for h in range(CHUNKS // 2, CHUNKS):
        image_first(h)
    p_sum[...] = jnp.zeros_like(p_sum)
    image_stage(0)
    when(relay & early, pl.semaphore_wait, fwd_ready, 1)
    when(relay & early, text_relay_stage, 0)
    when(relay & early, text_relay_stage, 1)
    when(middle, image_stage, 1)
    when(middle & first, image_stage, 2)
    tardy_first, tardy_second = early & first, early & (place == 1)
    when(edge & tardy_first, image_stage, 1)
    when(edge & tardy_first, image_stage, 2)
    text_stage(0)

    when(relay & late, text_relay_stage, 2)

    @pl.loop(0, 2 + z * (3 - z) // 2)
    def _(i):
        recent(jnp.where(i < 2, 1 - i, 2))

    when(edge & jnp.logical_not(tardy_first), image_stage, 1)
    when(edge & tardy_second, image_stage, 2)
    when(middle & jnp.logical_not(first), image_stage, 2)
    text_stage(1)
    when(edge, recent, 2)

    @pl.loop(0, 3)
    def _(i):
        older(2 - i)

    when(edge & jnp.logical_not(tardy_first | tardy_second), image_stage, 2)

    @pl.when(late & edge)
    def _():
        text_stage(2)
        oldest(1, 3)

    recent(3)
    older(3)

    @pl.when(late & middle)
    def _():
        text_stage(2)

    @pl.when(late)
    def _():
        oldest(0, jnp.where(middle, z, 1))


    when(first, pl.semaphore_wait, lane_ready, SLICES)
    slow = last | (late & (place == 30))
    hold = relay & (z == 3)

    def relay_step(n, here):
        when(relay & late & here, back_relay_stage, 2 - n)
        if n < 2:
            when(relay & soon & here, back_relay_stage, 1 - n)

    when(late, back_begin, 3)
    when(soon, back_begin, 2)
    relay_step(0, not_early)
    when(edge, far_start, 3)
    when(edge & jnp.logical_not(hold & late), far_start, 2)
    when(late & jnp.logical_not(last), back_pass, 2)
    when(middle, far_pass, 3)
    when(relay & early, pl.semaphore_wait, back_ready, 1)
    relay_step(0, early)
    when(edge & jnp.logical_not(hold), far_start, 1)
    when(jnp.logical_not(slow), back_pass, 1)
    relay_step(1, not_early)
    when(hold & late, far_start, 2)
    relay_step(2, not_early)
    when(middle, near_pass)
    relay_step(1, early)
    relay_step(2, early)
    when(hold, far_start, 1)
    when(middle, far_pass, 2)
    when(late & last, back_pass, 2)
    when(slow, back_pass, 1)
    when(edge, sum_arrival, 0)
    when(middle, sum_arrival, 1)

    def finish(which, h, total):
        r = rows(h)
        out_held[which, r] = undo(total, (image_ref, text_ref)[which][r])
        out_copy(which, h).start()

    def out_copy(which, h):
        r = rows(h)
        return pltpu.make_async_copy(out_held.at[which, r], (image_out, text_out)[which].at[r], out_sem.at[which])

    for h in range(CHUNKS):
        back_arrival(0, h)
        finish(1, h, p_sum[0, rows(h)] + p_recv[0, rows(h)].astype(F32))

    for h in range(CHUNKS):
        r = rows(h)

        @pl.when(edge)
        def _():
            far_arrival(0, h)
            finish(0, h, own_part(z, r) + far_in[z, r].astype(F32))

        @pl.when(middle)
        def _():
            near_arrival(1, h)
            far_arrival(1, h)
            finish(0, h, own_part(z, r) + near_in[z, r].astype(F32) + far_in[z, r].astype(F32))

    def sent(block, ssem):
        copy(block, block, ssem, img_rsem.at[0, 0], partner).wait_send()

    for which in range(2):
        pltpu.make_async_copy(out_held.at[which], (image_out, text_out)[which], out_sem.at[which]).wait()

    for d in range(3):
        used = late if d == 2 else True
        when(relay & used, lambda: text_relay(d).wait_send())
        when(relay & used, lambda: back_relay(d).wait_send())
        when((j >= 0) & used, sent, p_send.at[d], p_ssem.at[d])
        when((j >= 0) & used if d == 0 else jnp.logical_not(last) & used, sent, txt.at[d], txt_ssem.at[d])
        if d < 2:
            when(ante & (late if d == 1 else True), sent, txt.at[d], ante_ssem.at[d])

    for t in range(4):
        sent(img.at[k, spot(t)], img_psem.at[t])

    @pl.when(edge)
    def _():
        sent(img.at[k, spot(0)], img_fsem.at[0])
        for t in (1, 2, 3):
            sent(far_out.at[spot(t)], far_ssem.at[spot(t)])

    @pl.when(middle)
    def _():
        for t in (0, 1):
            sent(img.at[k, spot(t)], img_fsem.at[t])
        for t in (1, 2, 3):
            sent(img.at[k, spot(t)], img_nsem.at[t])
        for t in (2, 3):
            sent(far_out.at[spot(t)], far_ssem.at[spot(t)])
        sent(near_out, near_ssem)

    @pl.loop(0, 4)
    def _(s):
        sent(q_send.at[s], q_ssem.at[s])


def solution(mesh):
    blocks = mesh.shape["blk"]
    dma = pltpu.SemaphoreType.DMA
    block = (ROWS, WIDTH)

    def per_device(image_embeds, text_embeds):
        out = jax.ShapeDtypeStruct(block, BF16)
        anywhere = pl.BlockSpec(memory_space=pl.ANY)
        return pl.pallas_call(
            lambda *refs: kernel(blocks, *refs),
            out_shape=(out, out),
            in_specs=[anywhere] * 2,
            out_specs=(anywhere, anywhere),
            scratch_shapes=[
                pltpu.VMEM(block, BF16),
                pltpu.VMEM(block, BF16),
                dma((2,)),
                pltpu.VMEM((2,) + block, BF16),
                dma((2,)),
                pltpu.VMEM((2, 4) + block, BF16),
                pltpu.VMEM((4,) + block, BF16),
                pltpu.VMEM((2 * ROWS, 3 * ROWS), BF16),
                pltpu.VMEM((2, 4) + block, F32),
                pltpu.VMEM((4,) + block, F32),
                pltpu.VMEM((4,) + block, BF16),
                pltpu.VMEM((4,) + block, BF16),
                pltpu.VMEM((4,) + block, BF16),
                pltpu.VMEM(block, BF16),
                pltpu.VMEM((4,) + block, BF16),
                pltpu.VMEM((4,) + block, BF16),
                pltpu.VMEM((3,) + block, BF16),
                pltpu.VMEM((3,) + block, BF16),
                pltpu.VMEM((3, THIN, WIDTH), BF16),
                pltpu.VMEM((3, THIN, WIDTH), BF16),
                dma((3,)),
                dma((3, CHUNKS)),
                dma((4,)),
                dma((4,)),
                dma((4,)),
                dma((4, CHUNKS)),
                dma((4,)),
                dma((4,)),
                dma((4,)),
                dma((4,)),
                dma(()),
                dma((4, CHUNKS)),
                dma((4, CHUNKS)),
                dma((3,)),
                dma((3, CHUNKS)),
                dma((2,)),
                dma((3,)),
                dma((3,)),
                dma((3,)),
                dma((3,)),
                pltpu.SemaphoreType.REGULAR,
                pltpu.SemaphoreType.REGULAR,
                pltpu.SemaphoreType.REGULAR,
            ],
            compiler_params=pltpu.CompilerParams(
                collective_id=0, has_side_effects=True, vmem_limit_bytes=56 * 1024 * 1024
            ),
            name="pair_window",
        )(image_embeds, text_embeds)

    spec = P(("blk", "grp"), None)
    return jax.shard_map(
        per_device, mesh=mesh, in_specs=(spec, spec), out_specs=(spec, spec), check_vma=False
    )
```

```python
import jax
import jax.numpy as jnp
from jax import lax
from jax.experimental import pallas as pl
from jax.experimental.pallas import tpu as pltpu
from jax.sharding import PartitionSpec as P

MESH = pl.DeviceIdType.MESH
LOGIT_SCALE = 10.0
BIAS_LOGIT = -2.0
EPSILON = 1e-06
ROWS = 128
WIDTH = 1152
CHUNKS = 4
PIECE = ROWS // CHUNKS
SLICES = 8
THIN = ROWS // SLICES
RELAYS = ((26, 14, 17, 29, 2, 16, 7, 24), (9, 5, 22, 8, 6, 25, 15, 23))
COLS = 384
F32 = jnp.float32
BF16 = jnp.bfloat16


def unit_and_inverse(ref):
    wide = ref[...].astype(F32)
    length = jnp.sqrt(jnp.sum(wide * wide, axis=-1, keepdims=True) + EPSILON)
    inverse = 1.0 / length
    return wide * inverse, inverse


def undo(total, wide):
    wide = wide.astype(F32)
    inverse = 1.0 / jnp.sqrt(jnp.sum(wide * wide, axis=-1, keepdims=True) + EPSILON)
    unit = wide * inverse
    grad = LOGIT_SCALE * total
    inner = jnp.sum(unit * grad, axis=-1, keepdims=True)
    return ((grad - unit * inner) * inverse).astype(BF16)


def kernel(
    blocks,
    image_in, text_in, image_out, text_out,
    image_ref, text_ref, in_sem, out_held, out_sem,
    img, txt, wgt, q_sum, p_sum,
    q_send, q_recv, far_out, near_out, near_in, far_in, p_send, p_recv,
    fwd_hold, back_hold,
    txt_ssem, txt_rsem, img_fsem, img_nsem, img_psem, img_rsem, pair_rsem,
    q_ssem, q_rsem, far_ssem, near_ssem, near_rsem, far_rsem, p_ssem, p_rsem,
    ante_ssem, fwd_ssem, fwd_rsem, back_ssem, back_rsem, fwd_ready, back_ready, lane_ready,
):
    blk = lax.axis_index("blk")
    z = lax.axis_index("grp")
    k = lax.rem(blk, 2)
    j = 4 * k + z
    high = z // 2
    sign = 1 - 2 * high
    middle = (z == 1) | (z == 2)
    edge = (z == 0) | (z == 3)

    def spot(t):
        return 3 * high + sign * t

    column = blk // 2
    third = column // 32
    place = lax.rem(column, 32)
    first = place == 0
    last = place == 31
    ante = place == 30

    def relay_place(h):
        return RELAYS[0][h] + k * (RELAYS[1][h] - RELAYS[0][h])

    def at(hop, where):
        return (2 * (32 * lax.rem(third + hop, blocks // 64) + where) + k, z)

    role, relay = 0, False
    for h in range(SLICES):
        match = place == relay_place(h)
        role = role + jnp.where(match, h, 0)
        relay = relay | match
    next_first, own_first = at(1, 0), at(0, 0)
    prev_last, own_last, own_ante = at(blocks // 64 - 1, 31), at(0, 31), at(0, 30)

    partner = (blk + 1 - 2 * k, z)
    ahead = (lax.rem(blk + 2, blocks), z)
    behind = (lax.rem(blk + blocks - 2, blocks), z)
    far = (blk, z + sign)
    near = (blk, z - sign)

    def when(condition, run, *args):
        @pl.when(condition)
        def _():
            run(*args)

    def copy(src, dst, ssem, rsem, device):
        return pltpu.make_async_remote_copy(
            src_ref=src, dst_ref=dst, send_sem=ssem, recv_sem=rsem, device_id=device, device_id_type=MESH
        )

    def rows(h):
        return pl.ds(h * PIECE, PIECE)

    def thin(h):
        return pl.ds(pl.multiple_of(h * THIN, THIN), THIN)

    image_load = pltpu.make_async_copy(image_in, image_ref, in_sem.at[0])
    text_load = pltpu.make_async_copy(text_in, text_ref, in_sem.at[1])
    image_load.start()
    text_load.start()

    barrier = pltpu.get_barrier_semaphore()

    def greet(condition, devices):
        @pl.when(condition)
        def _():
            for device in devices:
                pl.semaphore_signal(barrier, inc=1, device_id=device, device_id_type=MESH)

    thirds = blocks // 64
    early, final = third == 0, third == thirds - 1
    not_early, not_final = jnp.logical_not(early), jnp.logical_not(final)
    past_relays = [at(thirds - 1, relay_place(h)) for h in range(SLICES)]
    coming_relays = [at(1, relay_place(h)) for h in range(SLICES)]
    own_relays = [at(0, relay_place(h)) for h in range(SLICES)]
    greet(relay, (own_last, own_ante))
    greet(first, own_relays)
    greet(first & early, past_relays)
    greet(last & not_final, coming_relays)
    greet(relay & not_final, (next_first,))
    greet(relay & early, (prev_last,))
    for device in (partner, far):
        pl.semaphore_signal(barrier, inc=1, device_id=device, device_id_type=MESH)
    greet(middle, (near,))
    greet(jnp.logical_not(first), (behind,))
    greet(jnp.logical_not(last), (ahead,))

    image_load.wait()
    unit, _ = unit_and_inverse(image_ref)
    img[k, z] = unit.astype(BF16)
    text_load.wait()
    unit, _ = unit_and_inverse(text_ref)
    txt[0] = unit.astype(BF16)

    answer_first, answer_last = first & not_early, last & final
    greeted = 4 + z * (3 - z) // 2 + jnp.where(last, SLICES - 1, 0) - jnp.where(first, 1, 0)
    greeted = greeted + jnp.where(answer_first | answer_last | ante, SLICES, 0)
    greeted = greeted + jnp.where(relay & final, 1, 0) + jnp.where(relay & not_early, 1, 0) + jnp.where(relay, 1, 0)
    pl.semaphore_wait(barrier, greeted)

    when(relay, lambda: pl.semaphore_signal(lane_ready, inc=1, device_id=own_first, device_id_type=MESH))

    @pl.when(answer_first)
    def _():
        for device in past_relays:
            pl.semaphore_signal(fwd_ready, inc=1, device_id=device, device_id_type=MESH)

    @pl.when(answer_last)
    def _():
        for device in coming_relays:
            pl.semaphore_signal(back_ready, inc=1, device_id=device, device_id_type=MESH)

    def image_copy(t, h, ssem, device):
        s = spot(t)
        ref = img.at[k, s, rows(h)]
        return copy(ref, ref, ssem.at[t], img_rsem.at[s, h], device)

    def to_partner(t, h):
        s = spot(t)
        ref = img.at[k, s, rows(h)]
        copy(ref, ref, img_psem.at[t], pair_rsem.at[s], partner).start()

    def image_arrival(s, h):
        ref = img.at[k, s, rows(h)]
        copy(ref, ref, img_psem.at[0], img_rsem.at[s, h], partner).wait_recv()

    def text_copy(d, h):
        return copy(
            txt.at[d, thin(h)], txt.at[d + 1, thin(h)], txt_ssem.at[d], txt_rsem.at[d, h // 2], ahead
        )

    def text_arrival(d, g):
        ref = txt.at[d + 1, rows(g)]
        copy(ref, ref, txt_ssem.at[d], txt_rsem.at[d, g], ahead).wait_recv()

    def back_arrival(d, g):
        ref = p_recv.at[d, rows(g)]
        copy(ref, ref, p_ssem.at[d], p_rsem.at[d, g], behind).wait_recv()

    def relay_copy(d, hold, h, ssem):
        return copy(txt.at[d, thin(h)], fwd_hold.at[hold], ssem, fwd_rsem.at[hold], at(0, relay_place(h)))

    def ante_copy(d, h):
        return relay_copy(d, d + 1, h, ante_ssem.at[d])

    def text_start(d, h):
        @pl.when(jnp.logical_not(last))
        def _():
            text_copy(d, h).start()

        if d == 0:
            @pl.when(last)
            def _():
                relay_copy(0, 0, h, txt_ssem.at[0]).start()

    def text_relay(d):
        return copy(
            fwd_hold.at[d], txt.at[d + 1, thin(role)], fwd_ssem.at[d], txt_rsem.at[d, role // 2], next_first
        )

    def text_relay_stage(d):
        copy(fwd_hold.at[d], fwd_hold.at[d], fwd_ssem.at[d], fwd_rsem.at[d], next_first).wait_recv()
        text_relay(d).start()

    for h in range(SLICES):
        when(ante, lambda h=h: ante_copy(0, h).start())

    for h in range(SLICES):
        text_start(0, h)

    def back_copy(d, h):
        return copy(p_send.at[d, thin(h)], p_recv.at[d, thin(h)], p_ssem.at[d], p_rsem.at[d, h // 2], behind)

    def back_start(d, h):
        @pl.when(first)
        def _():
            copy(
                p_send.at[d, thin(h)], back_hold.at[d], p_ssem.at[d], back_rsem.at[d], at(0, relay_place(h))
            ).start()

        @pl.when(jnp.logical_not(first))
        def _():
            back_copy(d, h).start()

    def back_relay(d):
        return copy(
            back_hold.at[d], p_recv.at[d, thin(role)], back_ssem.at[d], p_rsem.at[d, role // 2], prev_last
        )

    def back_relay_stage(d):
        copy(back_hold.at[d], back_hold.at[d], back_ssem.at[d], back_rsem.at[d], prev_last).wait_recv()
        back_relay(d).start()

    def far_copy(t, h, receiver):
        s = spot(t)
        sem = {"near": near_rsem, "far": far_rsem}[receiver]
        dst = {"near": near_in, "far": far_in}[receiver]
        return copy(far_out.at[s, rows(h)], dst.at[s, rows(h)], far_ssem.at[s], sem.at[s, h], far)

    def near_copy(h):
        s = spot(0)
        return copy(near_out.at[rows(h)], far_in.at[s, rows(h)], near_ssem, far_rsem.at[s, h], near)

    def near_arrival(t, h):
        s = spot(t)
        copy(far_out.at[s, rows(h)], near_in.at[s, rows(h)], far_ssem.at[s], near_rsem.at[s, h], far).wait_recv()

    def far_arrival(t, h):
        s = spot(t)
        copy(far_out.at[s, rows(h)], far_in.at[s, rows(h)], far_ssem.at[s], far_rsem.at[s, h], far).wait_recv()

    def sum_arrival(t):
        s = spot(t)
        copy(q_send.at[s], q_recv.at[s], q_ssem.at[s], q_rsem.at[s], partner).wait_recv()

    def own_part(s, r):
        return q_sum[k, s, r] + q_recv[s, r].astype(F32)

    def far_start(t):
        sum_arrival(t)
        s = spot(t)
        for h in range(CHUNKS):
            r = rows(h)
            far_out[s, r] = own_part(s, r).astype(BF16)
            far_copy(t, h, "near").start()

    def far_pass(t):
        sum_arrival(t)
        s = spot(t)
        for h in range(CHUNKS):
            r = rows(h)
            near_arrival(t, h)
            far_out[s, r] = (own_part(s, r) + near_in[s, r].astype(F32)).astype(BF16)
            far_copy(t, h, "far").start()

    def near_pass():
        sum_arrival(0)
        s = spot(0)
        for h in range(CHUNKS):
            r = rows(h)
            far_arrival(0, h)
            near_out[r] = (own_part(s, r) + far_in[s, r].astype(F32)).astype(BF16)
            near_copy(h).start()

    def back_begin(d):
        for h in range(SLICES):
            r = thin(h)
            p_send[d - 1, r] = p_sum[d, r].astype(BF16)
            back_start(d - 1, h)

    def back_pass(d):
        for g in range(CHUNKS):
            r = rows(g)
            back_arrival(d, g)
            p_send[d - 1, r] = (p_sum[d, r] + p_recv[d, r].astype(F32)).astype(BF16)
            back_start(d - 1, 2 * g)
            back_start(d - 1, 2 * g + 1)

    def image_first(h):
        @pl.when(edge)
        def _():
            image_copy(0, h, img_fsem, far).start()
            to_partner(0, h)

        @pl.when(middle)
        def _():
            image_copy(1, h, img_fsem, far).start()
            image_copy(1, h, img_nsem, near).start()
            to_partner(1, h)

    def image_stage(u):
        for h in range(CHUNKS):
            @pl.when(edge)
            def _():
                image_arrival(spot(u + 1), h)
                to_partner(u + 1, h)

            @pl.when(middle)
            def _():
                if u == 0:
                    image_arrival(spot(0), h)
                    image_copy(0, h, img_fsem, far).start()
                    to_partner(0, h)
                else:
                    image_arrival(spot(u + 1), h)
                    image_copy(u + 1, h, img_nsem, near).start()
                    to_partner(u + 1, h)

    def text_stage(u):
        for h in range(SLICES):
            if h % 2 == 0:
                text_arrival(u, h // 2)
            if u == 0:
                when(ante & (j >= 5), lambda h=h: ante_copy(1, h).start())
                when(jnp.logical_not(ante & (j >= 5)), text_start, 1, h)
            elif u == 1:
                @pl.when(j >= 5)
                def _():
                    text_start(2, h)

        if u == 0:
            @pl.when(ante & (j >= 5))
            def _():
                for h in range(SLICES):
                    text_start(1, h)

    def weights(logits, gap):
        logits = LOGIT_SCALE * logits + BIAS_LOGIT
        row = lax.broadcasted_iota(jnp.int32, logits.shape, 0)
        col = lax.broadcasted_iota(jnp.int32, logits.shape, 1)
        gap = gap + 8 * (col // ROWS) + 4 * (row // ROWS)
        match = (gap == 0) & (lax.rem(row, ROWS) == lax.rem(col, ROWS))
        weight = jax.nn.sigmoid(jnp.where(match, -logits, logits))
        weight = jnp.where(match, -weight, weight)
        return jnp.where((gap >= 0) & (gap <= 19), weight, 0.0).astype(BF16)

    NT = (((1,), (1,)), ((), ()))
    TN = (((0,), (0,)), ((), ()))

    def products(t, first_text, texts):
        s = spot(t)
        part_w = wgt.at[:, pl.ds(0, texts * ROWS)]
        near_texts = pl.ds(first_text, texts)
        pair = img[:, s].reshape(2 * ROWS, WIDTH)
        block = txt[near_texts].reshape(texts * ROWS, WIDTH)
        logits = lax.dot_general(pair, block, NT, preferred_element_type=F32)
        part_w[...] = weights(logits, 8 * first_text + s - j)
        for n in range(WIDTH // COLS):
            part = pl.ds(n * COLS, COLS)
            block = txt[near_texts, :, part].reshape(texts * ROWS, COLS)
            q = jnp.dot(part_w[...], block, preferred_element_type=F32).reshape(2, ROWS, COLS)
            pair = img[:, s, :, part].reshape(2 * ROWS, COLS)
            p = lax.dot_general(part_w[...], pair, TN, preferred_element_type=F32)
            if first_text == 0:
                q_sum[:, s, :, part] = q
            else:
                q_sum[:, s, :, part] += q
            p_sum[near_texts, :, part] += p.reshape(texts, ROWS, COLS)

    def recent(t):
        s = spot(t)
        ref = img.at[1 - k, s]
        copy(ref, ref, img_psem.at[t], pair_rsem.at[s], partner).wait_recv()
        products(t, 0, 2)

    def share(s):
        q_send[s] = q_sum[1 - k, s].astype(BF16)
        copy(q_send.at[s], q_recv.at[s], q_ssem.at[s], q_rsem.at[s], partner).start()

    def older(t):
        products(t, 2, 1)

        @pl.when((j < 5) | (spot(t) >= z))
        def _():
            share(spot(t))

    def oldest(start, stop):
        @pl.loop(start, stop)
        def _(s):
            old = weights(lax.dot_general(img[0, s], txt[3], NT, preferred_element_type=F32), 24 + s - j)
            q_sum[0, s] += jnp.dot(old, txt[3], preferred_element_type=F32)
            p_sum[3] += lax.dot_general(old, img[0, s], TN, preferred_element_type=F32)
            share(s)

    late = j >= 5
    soon = j < 5

    favoured = relay & final
    for h in range(CHUNKS // 2):
        when(jnp.logical_not(favoured), image_first, h)
    when(relay & not_final & not_early, pl.semaphore_wait, fwd_ready, 1)
    when(relay & not_early, text_relay_stage, 0)
    when(relay & not_early, text_relay_stage, 1)
    for h in range(CHUNKS // 2):
        when(favoured, image_first, h)
    for h in range(CHUNKS // 2, CHUNKS):
        image_first(h)
    p_sum[...] = jnp.zeros_like(p_sum)
    image_stage(0)
    when(relay & early, pl.semaphore_wait, fwd_ready, 1)
    when(relay & early, text_relay_stage, 0)
    when(relay & early, text_relay_stage, 1)
    when(middle, image_stage, 1)
    when(middle & first, image_stage, 2)
    tardy_first, tardy_second = early & first, early & (place == 1)
    when(edge & tardy_first, image_stage, 1)
    when(edge & tardy_first, image_stage, 2)
    text_stage(0)

    when(relay & late, text_relay_stage, 2)

    @pl.loop(0, 2 + z * (3 - z) // 2)
    def _(i):
        recent(jnp.where(i < 2, 1 - i, 2))

    when(edge & jnp.logical_not(tardy_first), image_stage, 1)
    when(edge & tardy_second, image_stage, 2)
    when(middle & jnp.logical_not(first), image_stage, 2)
    text_stage(1)
    when(edge, recent, 2)

    @pl.loop(0, 3)
    def _(i):
        older(2 - i)

    when(edge & jnp.logical_not(tardy_first | tardy_second), image_stage, 2)

    @pl.when(late & edge)
    def _():
        text_stage(2)
        oldest(1, 3)

    recent(3)
    older(3)

    @pl.when(late & middle)
    def _():
        text_stage(2)

    @pl.when(late)
    def _():
        oldest(0, jnp.where(middle, z, 1))


    when(first, pl.semaphore_wait, lane_ready, SLICES)
    slow = last | (late & (place == 30))
    hold = relay & (z == 3)

    def relay_step(n, here):
        when(relay & late & here, back_relay_stage, 2 - n)
        if n < 2:
            when(relay & soon & here, back_relay_stage, 1 - n)

    when(late, back_begin, 3)
    when(soon, back_begin, 2)
    relay_step(0, not_early)
    when(edge, far_start, 3)
    when(edge & jnp.logical_not(hold & late), far_start, 2)
    when(late & jnp.logical_not(last), back_pass, 2)
    when(middle, far_pass, 3)
    when(relay & early, pl.semaphore_wait, back_ready, 1)
    relay_step(0, early)
    when(edge & jnp.logical_not(hold), far_start, 1)
    when(jnp.logical_not(slow), back_pass, 1)
    relay_step(1, not_early)
    relay_step(2, not_early)
    when(hold & late, far_start, 2)
    when(middle, near_pass)
    relay_step(1, early)
    relay_step(2, early)
    when(hold, far_start, 1)
    when(middle, far_pass, 2)
    when(late & last, back_pass, 2)
    when(slow, back_pass, 1)
    when(edge, sum_arrival, 0)
    when(middle, sum_arrival, 1)

    def finish(which, h, total):
        r = rows(h)
        out_held[which, r] = undo(total, (image_ref, text_ref)[which][r])
        out_copy(which, h).start()

    def out_copy(which, h):
        r = rows(h)
        return pltpu.make_async_copy(out_held.at[which, r], (image_out, text_out)[which].at[r], out_sem.at[which])

    for h in range(CHUNKS):
        back_arrival(0, h)
        finish(1, h, p_sum[0, rows(h)] + p_recv[0, rows(h)].astype(F32))

    for h in range(CHUNKS):
        r = rows(h)

        @pl.when(edge)
        def _():
            far_arrival(0, h)
            finish(0, h, own_part(z, r) + far_in[z, r].astype(F32))

        @pl.when(middle)
        def _():
            near_arrival(1, h)
            far_arrival(1, h)
            finish(0, h, own_part(z, r) + near_in[z, r].astype(F32) + far_in[z, r].astype(F32))

    def sent(block, ssem):
        copy(block, block, ssem, img_rsem.at[0, 0], partner).wait_send()

    for which in range(2):
        pltpu.make_async_copy(out_held.at[which], (image_out, text_out)[which], out_sem.at[which]).wait()

    for d in range(3):
        used = late if d == 2 else True
        when(relay & used, lambda: text_relay(d).wait_send())
        when(relay & used, lambda: back_relay(d).wait_send())
        when((j >= 0) & used, sent, p_send.at[d], p_ssem.at[d])
        when((j >= 0) & used if d == 0 else jnp.logical_not(last) & used, sent, txt.at[d], txt_ssem.at[d])
        if d < 2:
            when(ante & (late if d == 1 else True), sent, txt.at[d], ante_ssem.at[d])

    for t in range(4):
        sent(img.at[k, spot(t)], img_psem.at[t])

    @pl.when(edge)
    def _():
        sent(img.at[k, spot(0)], img_fsem.at[0])
        for t in (1, 2, 3):
            sent(far_out.at[spot(t)], far_ssem.at[spot(t)])

    @pl.when(middle)
    def _():
        for t in (0, 1):
            sent(img.at[k, spot(t)], img_fsem.at[t])
        for t in (1, 2, 3):
            sent(img.at[k, spot(t)], img_nsem.at[t])
        for t in (2, 3):
            sent(far_out.at[spot(t)], far_ssem.at[spot(t)])
        sent(near_out, near_ssem)

    @pl.loop(0, 4)
    def _(s):
        sent(q_send.at[s], q_ssem.at[s])


def solution(mesh):
    blocks = mesh.shape["blk"]
    dma = pltpu.SemaphoreType.DMA
    block = (ROWS, WIDTH)

    def per_device(image_embeds, text_embeds):
        out = jax.ShapeDtypeStruct(block, BF16)
        anywhere = pl.BlockSpec(memory_space=pl.ANY)
        return pl.pallas_call(
            lambda *refs: kernel(blocks, *refs),
            out_shape=(out, out),
            in_specs=[anywhere] * 2,
            out_specs=(anywhere, anywhere),
            scratch_shapes=[
                pltpu.VMEM(block, BF16),
                pltpu.VMEM(block, BF16),
                dma((2,)),
                pltpu.VMEM((2,) + block, BF16),
                dma((2,)),
                pltpu.VMEM((2, 4) + block, BF16),
                pltpu.VMEM((4,) + block, BF16),
                pltpu.VMEM((2 * ROWS, 3 * ROWS), BF16),
                pltpu.VMEM((2, 4) + block, F32),
                pltpu.VMEM((4,) + block, F32),
                pltpu.VMEM((4,) + block, BF16),
                pltpu.VMEM((4,) + block, BF16),
                pltpu.VMEM((4,) + block, BF16),
                pltpu.VMEM(block, BF16),
                pltpu.VMEM((4,) + block, BF16),
                pltpu.VMEM((4,) + block, BF16),
                pltpu.VMEM((3,) + block, BF16),
                pltpu.VMEM((3,) + block, BF16),
                pltpu.VMEM((3, THIN, WIDTH), BF16),
                pltpu.VMEM((3, THIN, WIDTH), BF16),
                dma((3,)),
                dma((3, CHUNKS)),
                dma((4,)),
                dma((4,)),
                dma((4,)),
                dma((4, CHUNKS)),
                dma((4,)),
                dma((4,)),
                dma((4,)),
                dma((4,)),
                dma(()),
                dma((4, CHUNKS)),
                dma((4, CHUNKS)),
                dma((3,)),
                dma((3, CHUNKS)),
                dma((2,)),
                dma((3,)),
                dma((3,)),
                dma((3,)),
                dma((3,)),
                pltpu.SemaphoreType.REGULAR,
                pltpu.SemaphoreType.REGULAR,
                pltpu.SemaphoreType.REGULAR,
            ],
            compiler_params=pltpu.CompilerParams(
                collective_id=0, has_side_effects=True, vmem_limit_bytes=56 * 1024 * 1024
            ),
            name="pair_window",
        )(image_embeds, text_embeds)

    spec = P(("blk", "grp"), None)
    return jax.shard_map(
        per_device, mesh=mesh, in_specs=(spec, spec), out_specs=(spec, spec), check_vma=False
    )
```
